32 devices in a mesh: dp: 1 (over z), dcp: 32 (over y, x, core).
Axes of the slice: x: 4, y: 4, z: 1, core: 2. Of those that a mesh axis runs over, the one named last changes fastest.
The devices are a block of a 4x4x8 slice.
Arguments:
- q_abs: bfloat16 [64, 128, 576], P('dp', 'dcp')
- cache: bfloat16 [64, 16384, 576], P('dp', 'dcp')
- lengths: int32 [64], P('dp')
Outputs:
- output: bfloat16 [64, 128, 512], P('dp', 'dcp')
All inputs are finite; a program needn't handle non-finite values.
Results may differ from the reference program's by a relative error of at most 0.00794727.
Values are sent between devices in bfloat16 or wider.
A program may use at most 768 MiB of HBM per device.

```python
import jax
import jax.numpy as jnp
from jax import lax

HEADS = 128
KV_RANK = 512
ROPE = 64
QK_NOPE = 128
B = 64
S = 16384
NDEV = 32

WIDTH = KV_RANK + ROPE
SCALE = (QK_NOPE + ROPE) ** -0.5
BLOCK = S // NDEV
SEG = S // 32


def setup_inputs(seed: int = 0, part: int = 0) -> dict:
    key = jax.random.fold_in(jax.random.key(seed), part)
    kq, kc, kf, ks = jax.random.split(key, 4)
    q_abs = (jax.random.normal(kq, (B, HEADS, WIDTH), jnp.float32) * 0.6).astype(jnp.bfloat16)

    def draw(k):
        k1, k2, k3 = jax.random.split(k, 3)
        seg = jax.random.normal(k1, (32, KV_RANK), jnp.float32)
        lat = jax.random.normal(k2, (S, KV_RANK), jnp.float32) + jnp.repeat(seg, SEG, axis=0)
        rope = jax.random.normal(k3, (S, ROPE), jnp.float32) * 3.0
        return jnp.concatenate([lat, rope], axis=1).astype(jnp.bfloat16)

    cache = lax.map(draw, jax.random.split(kc, B))
    full = S - jax.random.randint(kf, (B,), 0, S // 64)
    short = jax.random.randint(ks, (B,), 1, S + 1)
    lengths = jnp.where(jnp.arange(B) % 2 == 0, full, short).astype(jnp.int32)
    return {'q_abs': q_abs, 'cache': cache, 'lengths': lengths}


def reference(q_abs, cache, lengths):
    pos = jnp.arange(S).reshape(NDEV, BLOCK)

    def one(args):
        qb, cb, lb = args
        cf = cb.astype(jnp.float32).reshape(NDEV, BLOCK, WIDTH)
        s = jnp.einsum('hk,ntk->nht', qb.astype(jnp.float32), cf) * SCALE
        valid = pos < lb
        s = jnp.where(valid[:, None, :], s, -jnp.inf)
        m = jnp.max(s, axis=2)
        m0 = jnp.where(jnp.isfinite(m), m, 0.0)
        p = jnp.exp(s - m0[:, :, None])
        l = jnp.sum(p, axis=2)
        pb = p.astype(jnp.bfloat16).astype(jnp.float32)
        pv = jnp.einsum('nht,ntc->nhc', pb, cf[:, :, :KV_RANK])
        has = l > 0.0
        l1 = jnp.where(has, l, 1.0)
        od = (pv / l1[:, :, None]).astype(jnp.bfloat16).astype(jnp.float32)
        lse_d = jnp.where(has, m0 + jnp.log(l1), -jnp.inf)
        mx = jnp.max(lse_d, axis=0)
        lse = mx + jnp.log(jnp.sum(jnp.exp(lse_d - mx[None, :]), axis=0))
        o = jnp.sum(jnp.exp(lse_d - lse[None, :])[:, :, None] * od, axis=0)
        return o.astype(jnp.bfloat16)

    return lax.map(one, (q_abs, cache, lengths))
```

```python
import functools

import jax
import jax.numpy as jnp
from jax import lax
from jax.experimental import pallas as pl
from jax.experimental.pallas import tpu as pltpu
from jax.sharding import PartitionSpec as P

ROPE = 64
SCALE = 192 ** -0.5
SIDE = 4
NS = 4
NB = 8
NEG = float('-inf')
F32 = jnp.float32
BF16 = jnp.bfloat16

LAG_P1F, LAG_P1R, LAG_FW, LAG_FR, LAG_C = 0, 1, 2, 3, 4
LAG_1, LAG_2, LAG_3, LAG_4, LAG_5 = 5, 6, 7, 8, 9


def softweights(parts):
    m = functools.reduce(jnp.maximum, parts)
    m0 = jnp.where(m == NEG, 0.0, m)
    ws = [jnp.exp(x - m0) for x in parts]
    tot = functools.reduce(jnp.add, ws)
    inv = 1.0 / jnp.where(tot == 0.0, 1.0, tot)
    return [w * inv for w in ws], m0 + jnp.log(tot)


def roll(x, shift):
    return pltpu.roll(x, shift % 128, 1)


def kernel(nc, len_ref, q_ref, cache_ref, out_ref,
           qraw, qm, qp, cbuf, cols, o_mine, o_send, o_recv, lse_own, lse_recv, lse_c, lse_r,
           fd_s, fd_r, m_s, m_r, acc, fd2_s, fd2_r, m2_s, m2_r, acc2,
           csem, s_p1, r_p1, s_p2, r_p2, s_qp, r_qp, s_o, r_o, s_fd, r_fd, s_m, r_m, s_fd2, r_fd2, s_m2, r_m2):
    me = lax.axis_index('dcp')
    core = me % 2
    x = (me // 2) % SIDE
    y = me // (2 * SIDE)
    nseq = q_ref.shape[0]
    sl = cbuf.shape[1]
    lat = out_ref.shape[2]
    lt = lat // 128
    half = NS // 2
    nt = qm.shape[2]
    ht = nt // 2

    def dev(xx, yy, cc):
        return {'dcp': (((yy + SIDE) % SIDE) * SIDE + (xx + SIDE) % SIDE) * 2 + cc}

    def small(ci, step):
        c = ci % 2
        return dev(x + (1 - c) * step, y + c * step, core)

    def big(ci, step):
        c = ci % 2
        return dev(x + c * step, y + (1 - c) * step, core)

    partner = dev(x, y, 1 - core)

    def first(ci):
        return (ci % 2) * (nseq // 2) + (ci // 2) * NS

    def rcopy(src, dst, ssem, rsem, to):
        return pltpu.make_async_remote_copy(src_ref=src, dst_ref=dst, send_sem=ssem, recv_sem=rsem, device_id=to,
                                            device_id_type=pl.DeviceIdType.MESH)

    def fetch(t):
        ci, s = t // NS, t % NS
        b = first(ci) + s
        return pltpu.make_async_copy(cache_ref.at[b], cbuf.at[t % NB], csem.at[t % NB])

    for t in range(NB):
        fetch(t).start()

    barrier = pltpu.get_barrier_semaphore()
    for to in (dev(x + 1, y, core), dev(x - 1, y, core), dev(x, y + 1, core), dev(x, y - 1, core), partner):
        pl.semaphore_signal(barrier, inc=1, device_id=to, device_id_type=pl.DeviceIdType.MESH)
    pl.semaphore_wait(barrier, 5)

    def p1(ci, d):
        sq = pl.ds(first(ci), NS)
        return rcopy(q_ref.at[sq], qraw.at[d, sq], s_p1.at[d], r_p1.at[ci, d], small(ci, 1 - 2 * d))

    def p1f(ci, d):
        sq = pl.ds(first(ci) + d * half, half)
        return rcopy(qraw.at[d, sq], qraw.at[2, sq], s_p1.at[2 + d], r_p1.at[ci, 2 + d], small(ci, 1 - 2 * d))

    def p2(ci, d):
        return rcopy(qm.at[0, ci], qm.at[3 - 2 * d, ci], s_p2.at[d], r_p2.at[ci, d], big(ci, 1 - 2 * d))

    def p2f(ci, d):
        tl = pl.ds(d * ht, ht)
        return rcopy(qm.at[3 - 2 * d, ci, tl], qm.at[2, ci, tl], s_p2.at[2 + d], r_p2.at[ci, 2 + d], big(ci, 1 - 2 * d))

    def toq(ci, slot):
        return rcopy(qm.at[slot, ci], qp.at[slot, ci], s_qp.at[slot], r_qp.at[ci, slot], partner)

    def too(ci):
        return rcopy(o_send.at[ci], o_recv.at[ci], s_o.at[0], r_o.at[ci, 0], partner)

    def tol(ci):
        return rcopy(lse_own.at[ci], lse_recv.at[ci], s_o.at[1], r_o.at[ci, 1], partner)

    def fd(ci, d):
        return rcopy(fd_s.at[d, ci], fd_r.at[d, ci], s_fd.at[d], r_fd.at[ci, d], big(ci, 1 - 2 * d))

    def mm(ci, d):
        return rcopy(m_s.at[d, ci], m_r.at[d, ci], s_m.at[d], r_m.at[ci, d], big(ci, 1 - 2 * d))

    def fd2(ci, d):
        return rcopy(fd2_s.at[d, ci], fd2_r.at[d, ci], s_fd2.at[d], r_fd2.at[ci, d], small(ci, 1 - 2 * d))

    def mm2(ci, d):
        return rcopy(m2_s.at[d, ci], m2_r.at[d, ci], s_m2.at[d], r_m2.at[ci, d], small(ci, 1 - 2 * d))

    def st_p1f(ci):
        for d in range(2):
            p1(ci, d).wait_recv()
            p1f(ci, d).start()

    def st_p1r(ci):
        for d in range(2):
            p1f(ci, d).wait_recv()
        ropes = []
        for s in range(NS):
            b = first(ci) + s
            rows = [q_ref[b], qraw[1, b], qraw[2, b], qraw[0, b]]
            rows = jnp.concatenate([r.astype(F32) for r in rows], axis=0)
            for l in range(lt):
                qm[0, ci, s * lt + l] = rows[:, l * 128:(l + 1) * 128].astype(BF16)
            ropes.append(rows[:, lat:lat + ROPE])
            if s % 2:
                qm[0, ci, NS * lt + s // 2] = jnp.concatenate(ropes[s - 1:s + 1], axis=1).astype(BF16)
        for d in range(2):
            p2(ci, d).start()
        toq(ci, 0).start()

    def st_fw(ci):
        for d in range(2):
            p2(ci, d).wait_recv()
            p2f(ci, d).start()
        toq(ci, 3).start()
        toq(ci, 1).start()

    def st_fr(ci):
        for d in range(2):
            p2f(ci, d).wait_recv()
        toq(ci, 2).start()

    lane128 = lax.broadcasted_iota(jnp.int32, (128, 128), 1)

    def st_c(ci):
        for slot in range(SIDE):
            toq(ci, slot).wait_recv()

        def pair(k, _):
            for u in range(2):
                s = 2 * k + u
                t = ci * NS + s
                b = first(ci) + s
                fetch(t).wait()
                tiles = []
                for l in range(lt):
                    i = s * lt + l
                    tiles.append(jnp.concatenate([qm[:, ci, i].reshape(64, 128), qp[:, ci, i].reshape(64, 128)], axis=0))
                i = NS * lt + k
                r = jnp.concatenate([qm[:, ci, i].reshape(64, 128), qp[:, ci, i].reshape(64, 128)], axis=0)
                tiles.append(r[:, u * ROPE:(u + 1) * ROPE])
                q = jnp.concatenate(tiles, axis=1)
                blk = cbuf.at[t % NB]
                sc = lax.dot_general(q, blk[...], (((1,), (1,)), ((), ())), preferred_element_type=F32) * SCALE
                pos = me * sl + lax.broadcasted_iota(jnp.int32, sc.shape, 1)
                sc = jnp.where(pos < len_ref[b], sc, NEG)
                m = jnp.max(sc, axis=1, keepdims=True)
                m0 = jnp.where(m == NEG, 0.0, m)
                p = jnp.exp(sc - m0)
                ls = jnp.sum(p, axis=1, keepdims=True)
                pv = lax.dot_general(p.astype(BF16), blk[:, :lat], (((1,), (0,)), ((), ())), preferred_element_type=F32)
                l1 = jnp.where(ls > 0.0, ls, 1.0)
                o = (pv * (1.0 / l1)).astype(BF16)
                lse = m0 + jnp.log(ls)
                cols[...] = jnp.where(lane128 == s, lse, cols[...])
                for slot in range(2 * SIDE):
                    to = o_mine if slot < SIDE else o_send
                    for l in range(lt):
                        to[ci, (s * SIDE + slot % SIDE) * lt + l] = o[slot * 16:(slot + 1) * 16, l * 128:(l + 1) * 128]

            for u in range(2):
                t = ci * NS + 2 * k + u + NB

                @pl.when(t < nc * NS)
                def _():
                    fetch(t).start()
            return 0

        lax.fori_loop(0, half, pair, 0)
        lse_own[ci] = cols[...].T[:8]
        too(ci).start()
        tol(ci).start()

    row8 = lax.broadcasted_iota(jnp.int32, (8, 128), 0)
    lane8 = lax.broadcasted_iota(jnp.int32, (8, 128), 1)

    def st_1(ci):
        too(ci).wait_recv()
        tol(ci).wait_recv()
        own = lse_own[ci]
        (wa, wb), lse = softweights([own, roll(lse_recv[ci], 64)])
        lse_c[ci] = lse
        wt = jnp.where(lane8 < 64, wa, roll(wb, 64)).T
        for d in range(2):
            fd_s[d, ci, NS * 2 * lt] = lse
        u = 2 * lt
        for s in range(NS):
            hf, sh = s // half, s % half
            for slot in range(SIDE):
                i = pl.ds((s * SIDE + slot) * lt, lt)
                ca = wt[slot * 16:(slot + 1) * 16, s:s + 1][None]
                cb = wt[64 + slot * 16:64 + (slot + 1) * 16, s:s + 1][None]
                v = (ca * o_mine[ci, i].astype(F32) + cb * o_recv[ci, i].astype(F32)).reshape(u, 8, 128)
                if slot == 0:
                    acc[ci, s * u:(s + 1) * u] = v
                elif slot == 2:
                    fd_s[hf, ci, sh * u:(sh + 1) * u] = v
                else:
                    d = 0 if slot == 1 else 1
                    if hf == 1 - d:
                        fd_s[d, ci, (half + sh) * u:(half + sh + 1) * u] = v
                    else:
                        m_s[d, ci, sh * u:(sh + 1) * u] = v
        for d in range(2):
            fd(ci, d).start()

    def st_2(ci):
        for d in range(2):
            fd(ci, d).wait_recv()
        u = 2 * lt
        left, right = fd_r[0, ci, NS * u], fd_r[1, ci, NS * u]
        far = jnp.where(lane8 < 32, roll(left, -16), roll(right, 16))
        (wa, wb), lse = softweights([lse_c[ci], far])
        wt = jnp.where(lane8 < 64, wa, roll(wb, 64)).T
        for d in range(2):
            m_s[d, ci, half * u] = lse
            for sh in range(half):
                s = d * half + sh
                r = 16 if d == 0 else 48
                ca = wt[r:r + 16, s:s + 1].reshape(1, 2, 8, 1)
                cb = wt[64 + r:80 + r, s:s + 1].reshape(1, 2, 8, 1)
                i = slice(sh * u, (sh + 1) * u)
                a = m_s[d, ci, i].reshape(lt, 2, 8, 128)
                f = fd_r[d, ci, i].reshape(lt, 2, 8, 128)
                m_s[d, ci, i] = (ca * a + cb * f).reshape(u, 8, 128)
            mm(ci, d).start()

    def st_3(ci):
        for d in range(2):
            mm(ci, d).wait_recv()
        u = 2 * lt
        left = roll(jnp.where(row8 < half, m_r[0, ci, half * u], fd_r[0, ci, NS * u]), -16)
        right = roll(jnp.where(row8 < half, fd_r[1, ci, NS * u], m_r[1, ci, half * u]), -48)
        (wo, wl, wr), lse = softweights([lse_c[ci], left, right])
        lse_r[ci] = lse
        for d in range(2):
            fd2_s[d, ci, NS * lt // 2] = lse
        wt = jnp.where(lane8 < 16, wo, jnp.where(lane8 < 32, roll(wl, 16), roll(wr, 32))).T
        res = []
        for s in range(NS):
            hf, sh = s // half, s % half
            im = slice(sh * u, (sh + 1) * u)
            idd = slice((half + sh) * u, (half + sh + 1) * u)
            lv = m_r[0, ci, im] if hf == 0 else fd_r[0, ci, idd]
            rv = fd_r[1, ci, idd] if hf == 0 else m_r[1, ci, im]
            vals = [acc[ci, s * u:(s + 1) * u], lv, rv]
            tot = 0.0
            for n, v in enumerate(vals):
                tot = tot + wt[n * 16:(n + 1) * 16, s:s + 1].reshape(1, 2, 8, 1) * v.reshape(lt, 2, 8, 128)
            res.append(tot.reshape(lt, 16, 128))
        for k in range(half):
            hf, kh = (2 * k) // half, k % (half // 2)
            for slot in range(SIDE):
                v = jnp.concatenate([res[2 * k][:, 4 * slot:4 * slot + 4], res[2 * k + 1][:, 4 * slot:4 * slot + 4]], axis=1)
                i = slice(kh * lt, (kh + 1) * lt)
                idd = slice((half // 2 + kh) * lt, (half // 2 + kh + 1) * lt)
                if slot == 0:
                    acc2[ci, k * lt:(k + 1) * lt] = v
                elif slot == 2:
                    fd2_s[hf, ci, i] = v
                else:
                    d = 0 if slot == 1 else 1
                    if hf == 1 - d:
                        fd2_s[d, ci, idd] = v
                    else:
                        m2_s[d, ci, i] = v
        for d in range(2):
            fd2(ci, d).start()

    def col2(wt, r, s):
        return jnp.concatenate([wt[r:r + 4, s:s + 1], wt[r:r + 4, s + 1:s + 2]], axis=0)[None]

    def st_4(ci):
        for d in range(2):
            fd2(ci, d).wait_recv()
        e = NS * lt // 2
        left, right = fd2_r[0, ci, e], fd2_r[1, ci, e]
        far = jnp.where(lane8 < 8, roll(left, -4), roll(right, 4))
        (wa, wb), lse = softweights([lse_r[ci], far])
        wt = jnp.where(lane8 < 64, wa, roll(wb, 64)).T
        for d in range(2):
            m2_s[d, ci, e // 2] = lse
            for kh in range(half // 2):
                s = d * half + 2 * kh
                r = 4 if d == 0 else 12
                i = slice(kh * lt, (kh + 1) * lt)
                m2_s[d, ci, i] = col2(wt, r, s) * m2_s[d, ci, i] + col2(wt, 64 + r, s) * fd2_r[d, ci, i]
            mm2(ci, d).start()

    def st_5(ci):
        for d in range(2):
            mm2(ci, d).wait_recv()
        e = NS * lt // 2
        left = roll(jnp.where(row8 < half, m2_r[0, ci, e // 2], fd2_r[0, ci, e]), -4)
        right = roll(jnp.where(row8 < half, fd2_r[1, ci, e], m2_r[1, ci, e // 2]), -12)
        (wo, wl, wr), _ = softweights([lse_r[ci], left, right])
        wt = jnp.where(lane8 < 16, wo, jnp.where(lane8 < 32, roll(wl, 16), roll(wr, 32))).T
        for k in range(half):
            hf, kh = (2 * k) // half, k % (half // 2)
            i = slice(kh * lt, (kh + 1) * lt)
            idd = slice((half // 2 + kh) * lt, (half // 2 + kh + 1) * lt)
            lv = m2_r[0, ci, i] if hf == 0 else fd2_r[0, ci, idd]
            rv = fd2_r[1, ci, idd] if hf == 0 else m2_r[1, ci, i]
            s = 2 * k
            tot = col2(wt, 0, s) * acc2[ci, k * lt:(k + 1) * lt] + col2(wt, 16, s) * lv + col2(wt, 32, s) * rv
            b = first(ci) + s
            for n in range(2):
                for l in range(lt):
                    out_ref[b + n, :, l * 128:(l + 1) * 128] = tot[l, 4 * n:4 * n + 4].astype(BF16)

    def send_p1(ci, _):
        for d in range(2):
            p1(ci, d).start()
        return 0

    cols[...] = jnp.zeros_like(cols)
    lax.fori_loop(0, nc, send_p1, 0)

    stages = [(LAG_P1F, st_p1f), (LAG_P1R, st_p1r), (LAG_FW, st_fw), (LAG_FR, st_fr), (LAG_C, st_c),
              (LAG_1, st_1), (LAG_2, st_2), (LAG_3, st_3), (LAG_4, st_4), (LAG_5, st_5)]

    def step(i, _):
        for lag, fn in stages:
            ci = i - lag

            @pl.when(jnp.logical_and(ci >= 0, ci < nc))
            def _():
                fn(ci)
        return 0

    lax.fori_loop(0, nc + LAG_5, step, 0)

    def drain(ref, sem):
        pltpu.make_async_copy(ref, ref, sem).wait()

    for d in range(2):
        drain(qraw.at[d], s_p1.at[d])
        drain(qraw.at[d, pl.ds(0, nseq // 2)], s_p1.at[2 + d])
        drain(qm.at[0], s_p2.at[d])
        drain(qm.at[0, :, pl.ds(0, ht)], s_p2.at[2 + d])
        drain(fd_s.at[d], s_fd.at[d])
        drain(m_s.at[d], s_m.at[d])
        drain(fd2_s.at[d], s_fd2.at[d])
        drain(m2_s.at[d], s_m2.at[d])
    for slot in range(SIDE):
        drain(qm.at[slot], s_qp.at[slot])
    drain(o_send, s_o.at[0])
    drain(lse_own, s_o.at[1])


def solution(mesh):
    assert mesh.shape['dcp'] == 2 * SIDE * SIDE

    def local(q, cache, lengths):
        nseq, heads, wd = q.shape
        sl = cache.shape[1]
        lat = wd - ROPE
        lt = lat // 128
        nc = nseq // NS
        nt = NS * lt + NS // 2
        vm = pltpu.VMEM
        dma = pltpu.SemaphoreType.DMA
        scratch = [
            vm((3, nseq, heads, wd), BF16),
            vm((SIDE, nc, nt, 16, 128), BF16),
            vm((SIDE, nc, nt, 16, 128), BF16),
            vm((NB, sl, wd), BF16),
            vm((128, 128), F32),
            vm((nc, NS * SIDE * lt, 16, 128), BF16),
            vm((nc, NS * SIDE * lt, 16, 128), BF16),
            vm((nc, NS * SIDE * lt, 16, 128), BF16),
            vm((nc, 8, 128), F32),
            vm((nc, 8, 128), F32),
            vm((nc, 8, 128), F32),
            vm((nc, 8, 128), F32),
            vm((2, nc, NS * 2 * lt + 1, 8, 128), F32),
            vm((2, nc, NS * 2 * lt + 1, 8, 128), F32),
            vm((2, nc, NS * lt + 1, 8, 128), F32),
            vm((2, nc, NS * lt + 1, 8, 128), F32),
            vm((nc, NS * 2 * lt, 8, 128), F32),
            vm((2, nc, NS * lt // 2 + 1, 8, 128), F32),
            vm((2, nc, NS * lt // 2 + 1, 8, 128), F32),
            vm((2, nc, NS * lt // 4 + 1, 8, 128), F32),
            vm((2, nc, NS * lt // 4 + 1, 8, 128), F32),
            vm((nc, NS * lt // 2, 8, 128), F32),
            dma((NB,)),
            dma((4,)), dma((nc, 4)),
            dma((4,)), dma((nc, 4)),
            dma((4,)), dma((nc, 4)),
            dma((2,)), dma((nc, 2)),
            dma((2,)), dma((nc, 2)),
            dma((2,)), dma((nc, 2)),
            dma((2,)), dma((nc, 2)),
            dma((2,)), dma((nc, 2)),
        ]
        return pl.pallas_call(
            functools.partial(kernel, nc),
            out_shape=jax.ShapeDtypeStruct((nseq, heads, lat), BF16),
            in_specs=[
                pl.BlockSpec(memory_space=pltpu.SMEM),
                pl.BlockSpec(memory_space=pltpu.VMEM),
                pl.BlockSpec(memory_space=pl.ANY),
            ],
            out_specs=pl.BlockSpec(memory_space=pltpu.VMEM),
            scratch_shapes=scratch,
            compiler_params=pltpu.CompilerParams(collective_id=0, has_side_effects=True, vmem_limit_bytes=67_000_000),
        )(lengths, q, cache)

    return jax.shard_map(local, mesh=mesh, in_specs=(P('dp', 'dcp', None), P('dp', 'dcp', None), P('dp')),
                         out_specs=P('dp', 'dcp', None), check_vma=False)
```

```python
import functools

import jax
import jax.numpy as jnp
from jax import lax
from jax.experimental import pallas as pl
from jax.experimental.pallas import tpu as pltpu
from jax.sharding import PartitionSpec as P

ROPE = 64
SCALE = 192 ** -0.5
SIDE = 4
NS = 4
NB = 8
NEG = float('-inf')
F32 = jnp.float32
BF16 = jnp.bfloat16

LAG_P1F, LAG_P1R, LAG_FW, LAG_FR, LAG_C = 0, 1, 2, 3, 4
LAG_1, LAG_2, LAG_3, LAG_4, LAG_5 = 5, 6, 7, 8, 9


def softweights(parts):
    m = functools.reduce(jnp.maximum, parts)
    m0 = jnp.where(m == NEG, 0.0, m)
    ws = [jnp.exp(x - m0) for x in parts]
    tot = functools.reduce(jnp.add, ws)
    inv = 1.0 / jnp.where(tot == 0.0, 1.0, tot)
    return [w * inv for w in ws], m0 + jnp.log(tot)


def roll(x, shift):
    return pltpu.roll(x, shift % 128, 1)


def kernel(nc, len_ref, q_ref, cache_ref, out_ref,
           qraw, qm, qp, cbuf, cols, o_mine, o_send, o_recv, lse_own, lse_recv, lse_c, lse_r,
           fd_s, fd_r, m_s, m_r, acc, fd2_s, fd2_r, m2_s, m2_r, acc2,
           csem, s_p1, r_p1, s_p2, r_p2, s_qp, r_qp, s_o, r_o, s_fd, r_fd, s_m, r_m, s_fd2, r_fd2, s_m2, r_m2):
    me = lax.axis_index('dcp')
    core = me % 2
    x = (me // 2) % SIDE
    y = me // (2 * SIDE)
    nseq = q_ref.shape[0]
    sl = cbuf.shape[2]
    lat = out_ref.shape[2]
    lt = lat // 128
    half = NS // 2
    nt = qm.shape[2]
    ht = nt // 2

    def dev(xx, yy, cc):
        return {'dcp': (((yy + SIDE) % SIDE) * SIDE + (xx + SIDE) % SIDE) * 2 + cc}

    def small(ci, step):
        c = ci % 2
        return dev(x + (1 - c) * step, y + c * step, core)

    def big(ci, step):
        c = ci % 2
        return dev(x + c * step, y + (1 - c) * step, core)

    partner = dev(x, y, 1 - core)

    def first(ci):
        return (ci % 2) * (nseq // 2) + (ci // 2) * NS

    def rcopy(src, dst, ssem, rsem, to):
        return pltpu.make_async_remote_copy(src_ref=src, dst_ref=dst, send_sem=ssem, recv_sem=rsem, device_id=to,
                                            device_id_type=pl.DeviceIdType.MESH)

    def fetch(t):
        ci, s = t // NS, t % NS
        b = first(ci) + s
        return pltpu.make_async_copy(cache_ref.at[b], cbuf.at[t % NB], csem.at[t % NB])

    for t in range(NB):
        fetch(t).start()

    barrier = pltpu.get_barrier_semaphore()
    for to in (dev(x + 1, y, core), dev(x - 1, y, core), dev(x, y + 1, core), dev(x, y - 1, core), partner):
        pl.semaphore_signal(barrier, inc=1, device_id=to, device_id_type=pl.DeviceIdType.MESH)
    pl.semaphore_wait(barrier, 5)

    def p1(ci, d):
        sq = pl.ds(first(ci), NS)
        return rcopy(q_ref.at[sq], qraw.at[d, sq], s_p1.at[d], r_p1.at[ci, d], small(ci, 1 - 2 * d))

    def p1f(ci, d):
        sq = pl.ds(first(ci) + d * half, half)
        return rcopy(qraw.at[d, sq], qraw.at[2, sq], s_p1.at[2 + d], r_p1.at[ci, 2 + d], small(ci, 1 - 2 * d))

    def p2(ci, d):
        return rcopy(qm.at[0, ci], qm.at[3 - 2 * d, ci], s_p2.at[d], r_p2.at[ci, d], big(ci, 1 - 2 * d))

    def p2f(ci, d):
        tl = pl.ds(d * ht, ht)
        return rcopy(qm.at[3 - 2 * d, ci, tl], qm.at[2, ci, tl], s_p2.at[2 + d], r_p2.at[ci, 2 + d], big(ci, 1 - 2 * d))

    def toq(ci, slot):
        return rcopy(qm.at[slot, ci], qp.at[slot, ci], s_qp.at[slot], r_qp.at[ci, slot], partner)

    def too(ci):
        return rcopy(o_send.at[ci], o_recv.at[ci], s_o.at[0], r_o.at[ci, 0], partner)

    def tol(ci):
        return rcopy(lse_own.at[ci], lse_recv.at[ci], s_o.at[1], r_o.at[ci, 1], partner)

    def fd(ci, d):
        return rcopy(fd_s.at[d, ci], fd_r.at[d, ci], s_fd.at[d], r_fd.at[ci, d], big(ci, 1 - 2 * d))

    def mm(ci, d):
        return rcopy(m_s.at[d, ci], m_r.at[d, ci], s_m.at[d], r_m.at[ci, d], big(ci, 1 - 2 * d))

    def fd2(ci, d):
        return rcopy(fd2_s.at[d, ci], fd2_r.at[d, ci], s_fd2.at[d], r_fd2.at[ci, d], small(ci, 1 - 2 * d))

    def mm2(ci, d):
        return rcopy(m2_s.at[d, ci], m2_r.at[d, ci], s_m2.at[d], r_m2.at[ci, d], small(ci, 1 - 2 * d))

    def st_p1f(ci):
        for d in range(2):
            p1(ci, d).wait_recv()
            p1f(ci, d).start()

    def st_p1r(ci):
        for d in range(2):
            p1f(ci, d).wait_recv()
        ropes = []
        for s in range(NS):
            b = first(ci) + s
            rows = [q_ref[b], qraw[1, b], qraw[2, b], qraw[0, b]]
            rows = jnp.concatenate([r.astype(F32) for r in rows], axis=0)
            for l in range(lt):
                qm[0, ci, s * lt + l] = rows[:, l * 128:(l + 1) * 128].astype(BF16)
            ropes.append(rows[:, lat:lat + ROPE])
            if s % 2:
                qm[0, ci, NS * lt + s // 2] = jnp.concatenate(ropes[s - 1:s + 1], axis=1).astype(BF16)
        for d in range(2):
            p2(ci, d).start()
        toq(ci, 0).start()

    def st_fw(ci):
        for d in range(2):
            p2(ci, d).wait_recv()
            p2f(ci, d).start()
        toq(ci, 3).start()
        toq(ci, 1).start()

    def st_fr(ci):
        for d in range(2):
            p2f(ci, d).wait_recv()
        toq(ci, 2).start()

    lane128 = lax.broadcasted_iota(jnp.int32, (128, 128), 1)

    def st_c(ci):
        for slot in range(SIDE):
            toq(ci, slot).wait_recv()

        def pair(k, _):
            for u in range(2):
                s = 2 * k + u
                t = ci * NS + s
                b = first(ci) + s
                fetch(t).wait()
                tiles = []
                for l in range(lt):
                    i = s * lt + l
                    tiles.append(jnp.concatenate([qm[:, ci, i].reshape(64, 128), qp[:, ci, i].reshape(64, 128)], axis=0))
                i = NS * lt + k
                r = jnp.concatenate([qm[:, ci, i].reshape(64, 128), qp[:, ci, i].reshape(64, 128)], axis=0)
                tiles.append(r[:, u * ROPE:(u + 1) * ROPE])
                q = jnp.concatenate(tiles, axis=1)
                blk = cbuf.at[t % NB]
                sc = lax.dot_general(q, blk[...], (((1,), (0,)), ((), ())), preferred_element_type=F32) * SCALE
                pos = me * sl + lax.broadcasted_iota(jnp.int32, sc.shape, 1)
                sc = jnp.where(pos < len_ref[b], sc, NEG)
                m = jnp.max(sc, axis=1, keepdims=True)
                m0 = jnp.where(m == NEG, 0.0, m)
                p = jnp.exp(sc - m0)
                ls = jnp.sum(p, axis=1, keepdims=True)
                pv = lax.dot_general(p.astype(BF16), blk[:lat], (((1,), (1,)), ((), ())), preferred_element_type=F32)
                l1 = jnp.where(ls > 0.0, ls, 1.0)
                o = (pv * (1.0 / l1)).astype(BF16)
                lse = m0 + jnp.log(ls)
                cols[...] = jnp.where(lane128 == s, lse, cols[...])
                for slot in range(2 * SIDE):
                    to = o_mine if slot < SIDE else o_send
                    for l in range(lt):
                        to[ci, (s * SIDE + slot % SIDE) * lt + l] = o[slot * 16:(slot + 1) * 16, l * 128:(l + 1) * 128]

            for u in range(2):
                t = ci * NS + 2 * k + u + NB

                @pl.when(t < nc * NS)
                def _():
                    fetch(t).start()
            return 0

        lax.fori_loop(0, half, pair, 0)
        lse_own[ci] = cols[...].T[:8]
        too(ci).start()
        tol(ci).start()

    row8 = lax.broadcasted_iota(jnp.int32, (8, 128), 0)
    lane8 = lax.broadcasted_iota(jnp.int32, (8, 128), 1)

    def st_1(ci):
        too(ci).wait_recv()
        tol(ci).wait_recv()
        own = lse_own[ci]
        (wa, wb), lse = softweights([own, roll(lse_recv[ci], 64)])
        lse_c[ci] = lse
        wt = jnp.where(lane8 < 64, wa, roll(wb, 64)).T
        for d in range(2):
            fd_s[d, ci, NS * 2 * lt] = lse
        u = 2 * lt
        for s in range(NS):
            hf, sh = s // half, s % half
            for slot in range(SIDE):
                i = pl.ds((s * SIDE + slot) * lt, lt)
                ca = wt[slot * 16:(slot + 1) * 16, s:s + 1][None]
                cb = wt[64 + slot * 16:64 + (slot + 1) * 16, s:s + 1][None]
                v = (ca * o_mine[ci, i].astype(F32) + cb * o_recv[ci, i].astype(F32)).reshape(u, 8, 128)
                if slot == 0:
                    acc[ci, s * u:(s + 1) * u] = v
                elif slot == 2:
                    fd_s[hf, ci, sh * u:(sh + 1) * u] = v
                else:
                    d = 0 if slot == 1 else 1
                    if hf == 1 - d:
                        fd_s[d, ci, (half + sh) * u:(half + sh + 1) * u] = v
                    else:
                        m_s[d, ci, sh * u:(sh + 1) * u] = v
        for d in range(2):
            fd(ci, d).start()

    def st_2(ci):
        for d in range(2):
            fd(ci, d).wait_recv()
        u = 2 * lt
        left, right = fd_r[0, ci, NS * u], fd_r[1, ci, NS * u]
        far = jnp.where(lane8 < 32, roll(left, -16), roll(right, 16))
        (wa, wb), lse = softweights([lse_c[ci], far])
        wt = jnp.where(lane8 < 64, wa, roll(wb, 64)).T
        for d in range(2):
            m_s[d, ci, half * u] = lse
            for sh in range(half):
                s = d * half + sh
                r = 16 if d == 0 else 48
                ca = wt[r:r + 16, s:s + 1].reshape(1, 2, 8, 1)
                cb = wt[64 + r:80 + r, s:s + 1].reshape(1, 2, 8, 1)
                i = slice(sh * u, (sh + 1) * u)
                a = m_s[d, ci, i].reshape(lt, 2, 8, 128)
                f = fd_r[d, ci, i].reshape(lt, 2, 8, 128)
                m_s[d, ci, i] = (ca * a + cb * f).reshape(u, 8, 128)
            mm(ci, d).start()

    def st_3(ci):
        for d in range(2):
            mm(ci, d).wait_recv()
        u = 2 * lt
        left = roll(jnp.where(row8 < half, m_r[0, ci, half * u], fd_r[0, ci, NS * u]), -16)
        right = roll(jnp.where(row8 < half, fd_r[1, ci, NS * u], m_r[1, ci, half * u]), -48)
        (wo, wl, wr), lse = softweights([lse_c[ci], left, right])
        lse_r[ci] = lse
        for d in range(2):
            fd2_s[d, ci, NS * lt // 2] = lse
        wt = jnp.where(lane8 < 16, wo, jnp.where(lane8 < 32, roll(wl, 16), roll(wr, 32))).T
        res = []
        for s in range(NS):
            hf, sh = s // half, s % half
            im = slice(sh * u, (sh + 1) * u)
            idd = slice((half + sh) * u, (half + sh + 1) * u)
            lv = m_r[0, ci, im] if hf == 0 else fd_r[0, ci, idd]
            rv = fd_r[1, ci, idd] if hf == 0 else m_r[1, ci, im]
            vals = [acc[ci, s * u:(s + 1) * u], lv, rv]
            tot = 0.0
            for n, v in enumerate(vals):
                tot = tot + wt[n * 16:(n + 1) * 16, s:s + 1].reshape(1, 2, 8, 1) * v.reshape(lt, 2, 8, 128)
            res.append(tot.reshape(lt, 16, 128))
        for k in range(half):
            hf, kh = (2 * k) // half, k % (half // 2)
            for slot in range(SIDE):
                v = jnp.concatenate([res[2 * k][:, 4 * slot:4 * slot + 4], res[2 * k + 1][:, 4 * slot:4 * slot + 4]], axis=1)
                i = slice(kh * lt, (kh + 1) * lt)
                idd = slice((half // 2 + kh) * lt, (half // 2 + kh + 1) * lt)
                if slot == 0:
                    acc2[ci, k * lt:(k + 1) * lt] = v
                elif slot == 2:
                    fd2_s[hf, ci, i] = v
                else:
                    d = 0 if slot == 1 else 1
                    if hf == 1 - d:
                        fd2_s[d, ci, idd] = v
                    else:
                        m2_s[d, ci, i] = v
        for d in range(2):
            fd2(ci, d).start()

    def col2(wt, r, s):
        return jnp.concatenate([wt[r:r + 4, s:s + 1], wt[r:r + 4, s + 1:s + 2]], axis=0)[None]

    def st_4(ci):
        for d in range(2):
            fd2(ci, d).wait_recv()
        e = NS * lt // 2
        left, right = fd2_r[0, ci, e], fd2_r[1, ci, e]
        far = jnp.where(lane8 < 8, roll(left, -4), roll(right, 4))
        (wa, wb), lse = softweights([lse_r[ci], far])
        wt = jnp.where(lane8 < 64, wa, roll(wb, 64)).T
        for d in range(2):
            m2_s[d, ci, e // 2] = lse
            for kh in range(half // 2):
                s = d * half + 2 * kh
                r = 4 if d == 0 else 12
                i = slice(kh * lt, (kh + 1) * lt)
                m2_s[d, ci, i] = col2(wt, r, s) * m2_s[d, ci, i] + col2(wt, 64 + r, s) * fd2_r[d, ci, i]
            mm2(ci, d).start()

    def st_5(ci):
        for d in range(2):
            mm2(ci, d).wait_recv()
        e = NS * lt // 2
        left = roll(jnp.where(row8 < half, m2_r[0, ci, e // 2], fd2_r[0, ci, e]), -4)
        right = roll(jnp.where(row8 < half, fd2_r[1, ci, e], m2_r[1, ci, e // 2]), -12)
        (wo, wl, wr), _ = softweights([lse_r[ci], left, right])
        wt = jnp.where(lane8 < 16, wo, jnp.where(lane8 < 32, roll(wl, 16), roll(wr, 32))).T
        for k in range(half):
            hf, kh = (2 * k) // half, k % (half // 2)
            i = slice(kh * lt, (kh + 1) * lt)
            idd = slice((half // 2 + kh) * lt, (half // 2 + kh + 1) * lt)
            lv = m2_r[0, ci, i] if hf == 0 else fd2_r[0, ci, idd]
            rv = fd2_r[1, ci, idd] if hf == 0 else m2_r[1, ci, i]
            s = 2 * k
            tot = col2(wt, 0, s) * acc2[ci, k * lt:(k + 1) * lt] + col2(wt, 16, s) * lv + col2(wt, 32, s) * rv
            b = first(ci) + s
            for n in range(2):
                for l in range(lt):
                    out_ref[b + n, :, l * 128:(l + 1) * 128] = tot[l, 4 * n:4 * n + 4].astype(BF16)

    def send_p1(ci, _):
        for d in range(2):
            p1(ci, d).start()
        return 0

    cols[...] = jnp.zeros_like(cols)
    lax.fori_loop(0, nc, send_p1, 0)

    stages = [(LAG_P1F, st_p1f), (LAG_P1R, st_p1r), (LAG_FW, st_fw), (LAG_FR, st_fr), (LAG_C, st_c),
              (LAG_1, st_1), (LAG_2, st_2), (LAG_3, st_3), (LAG_4, st_4), (LAG_5, st_5)]

    def step(i, _):
        for lag, fn in stages:
            ci = i - lag

            @pl.when(jnp.logical_and(ci >= 0, ci < nc))
            def _():
                fn(ci)
        return 0

    lax.fori_loop(0, nc + LAG_5, step, 0)

    def drain(ref, sem):
        pltpu.make_async_copy(ref, ref, sem).wait()

    for d in range(2):
        drain(qraw.at[d], s_p1.at[d])
        drain(qraw.at[d, pl.ds(0, nseq // 2)], s_p1.at[2 + d])
        drain(qm.at[0], s_p2.at[d])
        drain(qm.at[0, :, pl.ds(0, ht)], s_p2.at[2 + d])
        drain(fd_s.at[d], s_fd.at[d])
        drain(m_s.at[d], s_m.at[d])
        drain(fd2_s.at[d], s_fd2.at[d])
        drain(m2_s.at[d], s_m2.at[d])
    for slot in range(SIDE):
        drain(qm.at[slot], s_qp.at[slot])
    drain(o_send, s_o.at[0])
    drain(lse_own, s_o.at[1])


def solution(mesh):
    assert mesh.shape['dcp'] == 2 * SIDE * SIDE

    def local(q, cache, lengths):
        nseq, heads, wd = q.shape
        sl = cache.shape[1]
        lat = wd - ROPE
        lt = lat // 128
        nc = nseq // NS
        nt = NS * lt + NS // 2
        vm = pltpu.VMEM
        dma = pltpu.SemaphoreType.DMA
        scratch = [
            vm((3, nseq, heads, wd), BF16),
            vm((SIDE, nc, nt, 16, 128), BF16),
            vm((SIDE, nc, nt, 16, 128), BF16),
            vm((NB, wd, sl), BF16),
            vm((128, 128), F32),
            vm((nc, NS * SIDE * lt, 16, 128), BF16),
            vm((nc, NS * SIDE * lt, 16, 128), BF16),
            vm((nc, NS * SIDE * lt, 16, 128), BF16),
            vm((nc, 8, 128), F32),
            vm((nc, 8, 128), F32),
            vm((nc, 8, 128), F32),
            vm((nc, 8, 128), F32),
            vm((2, nc, NS * 2 * lt + 1, 8, 128), F32),
            vm((2, nc, NS * 2 * lt + 1, 8, 128), F32),
            vm((2, nc, NS * lt + 1, 8, 128), F32),
            vm((2, nc, NS * lt + 1, 8, 128), F32),
            vm((nc, NS * 2 * lt, 8, 128), F32),
            vm((2, nc, NS * lt // 2 + 1, 8, 128), F32),
            vm((2, nc, NS * lt // 2 + 1, 8, 128), F32),
            vm((2, nc, NS * lt // 4 + 1, 8, 128), F32),
            vm((2, nc, NS * lt // 4 + 1, 8, 128), F32),
            vm((nc, NS * lt // 2, 8, 128), F32),
            dma((NB,)),
            dma((4,)), dma((nc, 4)),
            dma((4,)), dma((nc, 4)),
            dma((4,)), dma((nc, 4)),
            dma((2,)), dma((nc, 2)),
            dma((2,)), dma((nc, 2)),
            dma((2,)), dma((nc, 2)),
            dma((2,)), dma((nc, 2)),
            dma((2,)), dma((nc, 2)),
        ]
        return pl.pallas_call(
            functools.partial(kernel, nc),
            out_shape=jax.ShapeDtypeStruct((nseq, heads, lat), BF16),
            in_specs=[
                pl.BlockSpec(memory_space=pltpu.SMEM),
                pl.BlockSpec(memory_space=pltpu.VMEM),
                pl.BlockSpec(memory_space=pl.ANY),
            ],
            out_specs=pl.BlockSpec(memory_space=pltpu.VMEM),
            scratch_shapes=scratch,
            compiler_params=pltpu.CompilerParams(collective_id=0, has_side_effects=True, vmem_limit_bytes=67_000_000),
        )(lengths, q, jnp.swapaxes(cache, 1, 2))

    return jax.shard_map(local, mesh=mesh, in_specs=(P('dp', 'dcp', None), P('dp', 'dcp', None), P('dp')),
                         out_specs=P('dp', 'dcp', None), check_vma=False)
```

```python
import functools

import jax
import jax.numpy as jnp
from jax import lax
from jax.experimental import pallas as pl
from jax.experimental.pallas import tpu as pltpu
from jax.sharding import PartitionSpec as P

ROPE = 64
SCALE = 192 ** -0.5
SIDE = 4
NS = 4
NB = 8
NEG = float('-inf')
LOG2E = 1.4426950408889634
LN2 = 0.6931471805599453
F32 = jnp.float32
BF16 = jnp.bfloat16

LAG_P1R, LAG_FW, LAG_FR, LAG_C = 0, 4, 8, 9
LAG_1, LAG_2, LAG_3, LAG_4, LAG_5 = 10, 14, 18, 21, 24


def softweights(parts):
    m = functools.reduce(jnp.maximum, parts)
    m0 = jnp.where(m == NEG, 0.0, m)
    ws = [jnp.exp(x - m0) for x in parts]
    tot = functools.reduce(jnp.add, ws)
    inv = 1.0 / jnp.where(tot == 0.0, 1.0, tot)
    return [w * inv for w in ws], m0 + jnp.log(tot)


def roll(x, shift):
    return pltpu.roll(x, shift % 128, 1)


def kernel(nc, len_ref, q_ref, cache_ref, out_ref,
           qraw, qm, qp, cbuf, cols, o_mine, o_send, o_recv, lse_own, lse_recv, lse_c, lse_r,
           fd_s, fd_r, m_s, m_r, acc, fd2_s, fd2_r, m2_s, m2_r, acc2,
           csem, s_p1, r_p1, s_p2, r_p2, s_qp, r_qp, s_o, r_o, s_fd, r_fd, s_m, r_m, s_fd2, r_fd2, s_m2, r_m2):
    me = lax.axis_index('dcp')
    core = me % 2
    x = (me // 2) % SIDE
    y = me // (2 * SIDE)
    nseq = q_ref.shape[0]
    sl = cbuf.shape[2]
    lat = out_ref.shape[2]
    lt = lat // 128
    half = NS // 2
    nt = qm.shape[2]
    ht = nt // 2

    def dev(xx, yy, cc):
        return {'dcp': (((yy + SIDE) % SIDE) * SIDE + (xx + SIDE) % SIDE) * 2 + cc}

    def small(ci, step):
        c = ci % 2
        return dev(x + (1 - c) * step, y + c * step, core)

    def big(ci, step):
        c = ci % 2
        return dev(x + c * step, y + (1 - c) * step, core)

    partner = dev(x, y, 1 - core)

    def first(ci):
        return (ci % 2) * (nseq // 2) + (ci // 2) * NS

    def rcopy(src, dst, ssem, rsem, to):
        return pltpu.make_async_remote_copy(src_ref=src, dst_ref=dst, send_sem=ssem, recv_sem=rsem, device_id=to,
                                            device_id_type=pl.DeviceIdType.MESH)

    def fetch(t):
        ci, s = t // NS, t % NS
        b = first(ci) + s
        return pltpu.make_async_copy(cache_ref.at[b], cbuf.at[t % NB], csem.at[t % NB])

    for t in range(NB):
        fetch(t).start()

    barrier = pltpu.get_barrier_semaphore()
    for to in (dev(x + 1, y, core), dev(x - 1, y, core), dev(x, y + 1, core), dev(x, y - 1, core), partner):
        pl.semaphore_signal(barrier, inc=1, device_id=to, device_id_type=pl.DeviceIdType.MESH)
    pl.semaphore_wait(barrier, 5)

    def p1(ci, d):
        sq = pl.ds(first(ci), NS)
        return rcopy(q_ref.at[sq], qraw.at[d, sq], s_p1.at[d], r_p1.at[ci, d], small(ci, 1 - 2 * d))

    def p1f(ci, d):
        sq = pl.ds(first(ci) + d * half, half)
        return rcopy(qraw.at[d, sq], qraw.at[2, sq], s_p1.at[2 + d], r_p1.at[ci, 2 + d], small(ci, 1 - 2 * d))

    def p2(ci, d):
        return rcopy(qm.at[0, ci], qm.at[3 - 2 * d, ci], s_p2.at[d], r_p2.at[ci, d], big(ci, 1 - 2 * d))

    def p2f(ci, d):
        tl = pl.ds(d * ht, ht)
        return rcopy(qm.at[3 - 2 * d, ci, tl], qm.at[2, ci, tl], s_p2.at[2 + d], r_p2.at[ci, 2 + d], big(ci, 1 - 2 * d))

    def toq(ci, slot):
        return rcopy(qm.at[slot, ci], qp.at[slot, ci], s_qp.at[slot], r_qp.at[ci, slot], partner)

    def too(ci):
        return rcopy(o_send.at[ci], o_recv.at[ci], s_o.at[0], r_o.at[ci, 0], partner)

    def tol(ci):
        return rcopy(lse_own.at[ci], lse_recv.at[ci], s_o.at[1], r_o.at[ci, 1], partner)

    def fd(ci, d):
        return rcopy(fd_s.at[d, ci], fd_r.at[d, ci], s_fd.at[d], r_fd.at[ci, d], big(ci, 1 - 2 * d))

    def mm(ci, d):
        return rcopy(m_s.at[d, ci], m_r.at[d, ci], s_m.at[d], r_m.at[ci, d], big(ci, 1 - 2 * d))

    def fd2(ci, d):
        return rcopy(fd2_s.at[d, ci], fd2_r.at[d, ci], s_fd2.at[d], r_fd2.at[ci, d], small(ci, 1 - 2 * d))

    def mm2(ci, d):
        return rcopy(m2_s.at[d, ci], m2_r.at[d, ci], s_m2.at[d], r_m2.at[ci, d], small(ci, 1 - 2 * d))

    def st_p1f(ci):
        for d in range(2):
            p1(ci, d).wait_recv()
            p1f(ci, d).start()

    def st_p1r(ci):
        for d in range(2):
            p1f(ci, d).wait_recv()
        ropes = []
        for s in range(NS):
            b = first(ci) + s
            rows = [q_ref[b], qraw[1, b], qraw[2, b], qraw[0, b]]
            rows = jnp.concatenate([r.astype(F32) for r in rows], axis=0)
            for l in range(lt):
                qm[0, ci, s * lt + l] = rows[:, l * 128:(l + 1) * 128].astype(BF16)
            ropes.append(rows[:, lat:lat + ROPE])
            if s % 2:
                qm[0, ci, NS * lt + s // 2] = jnp.concatenate(ropes[s - 1:s + 1], axis=1).astype(BF16)
        for d in range(2):
            p2(ci, d).start()
        toq(ci, 0).start()

    def st_fw(ci):
        for d in range(2):
            p2(ci, d).wait_recv()
            p2f(ci, d).start()
        toq(ci, 3).start()
        toq(ci, 1).start()

    def st_fr(ci):
        for d in range(2):
            p2f(ci, d).wait_recv()
        toq(ci, 2).start()

    lane128 = lax.broadcasted_iota(jnp.int32, (128, 128), 1)

    def st_c(ci):
        for slot in range(SIDE):
            toq(ci, slot).wait_recv()

        for s in range(NS):
            fetch(ci * NS + s).wait()

        def block(s):
            return cbuf.at[(ci * NS + s) % NB]

        def scores(s):
            idx = [s * lt + l for l in range(lt)] + [NS * lt + s // 2]
            tiles = [jnp.concatenate([qm[:, ci, i].reshape(64, 128), qp[:, ci, i].reshape(64, 128)], axis=0) for i in idx]
            tiles[lt] = tiles[lt][:, s % 2 * ROPE:(s % 2 + 1) * ROPE]
            q = jnp.concatenate(tiles, axis=1)
            return lax.dot_general(q, block(s)[...], (((1,), (0,)), ((), ())), preferred_element_type=F32)

        def attend(s, sc):
            sc = jnp.where(pos < len_ref[first(ci) + s], sc * (SCALE * LOG2E), NEG)
            m = jnp.max(sc, axis=1, keepdims=True)
            m0 = jnp.where(m == NEG, 0.0, m)
            p = jnp.exp2(sc - m0)
            ls = jnp.sum(p, axis=1, keepdims=True)
            pv = lax.dot_general(p.astype(BF16), block(s)[:lat], (((1,), (1,)), ((), ())), preferred_element_type=F32)
            l1 = jnp.where(ls > 0.0, ls, 1.0)
            o = (pv * (1.0 / l1)).astype(BF16)
            for slot in range(2 * SIDE):
                to = o_mine if slot < SIDE else o_send
                for l in range(lt):
                    to[ci, (s * SIDE + slot % SIDE) * lt + l] = o[slot * 16:(slot + 1) * 16, l * 128:(l + 1) * 128]
            return m0 * LN2 + jnp.log(ls)

        pos = me * sl + lax.broadcasted_iota(jnp.int32, (1, sl), 1)
        sc = scores(0)
        for s in range(NS):
            after = scores(s + 1) if s + 1 < NS else None
            lse = attend(s, sc)
            cols[...] = jnp.where(lane128 == s, lse, cols[...])
            sc = after

        for s in range(NS):
            t = (ci + NB // NS) * NS + s

            @pl.when(t < nc * NS)
            def _():
                fetch(t).start()

        lse_own[ci] = cols[...].T[:8]
        too(ci).start()
        tol(ci).start()

    row8 = lax.broadcasted_iota(jnp.int32, (8, 128), 0)
    lane8 = lax.broadcasted_iota(jnp.int32, (8, 128), 1)

    def st_1(ci):
        too(ci).wait_recv()
        tol(ci).wait_recv()
        own = lse_own[ci]
        (wa, wb), lse = softweights([own, roll(lse_recv[ci], 64)])
        lse_c[ci] = lse
        wt = jnp.where(lane8 < 64, wa, roll(wb, 64)).T
        for d in range(2):
            fd_s[d, ci, NS * 2 * lt] = lse
        u = 2 * lt
        for s in range(NS):
            hf, sh = s // half, s % half
            for slot in range(SIDE):
                i = pl.ds((s * SIDE + slot) * lt, lt)
                ca = wt[slot * 16:(slot + 1) * 16, s:s + 1][None]
                cb = wt[64 + slot * 16:64 + (slot + 1) * 16, s:s + 1][None]
                v = (ca * o_mine[ci, i].astype(F32) + cb * o_recv[ci, i].astype(F32)).reshape(u, 8, 128)
                if slot == 0:
                    acc[ci, s * u:(s + 1) * u] = v
                elif slot == 2:
                    fd_s[hf, ci, sh * u:(sh + 1) * u] = v
                else:
                    d = 0 if slot == 1 else 1
                    if hf == 1 - d:
                        fd_s[d, ci, (half + sh) * u:(half + sh + 1) * u] = v
                    else:
                        m_s[d, ci, sh * u:(sh + 1) * u] = v
        for d in range(2):
            fd(ci, d).start()

    def st_2(ci):
        for d in range(2):
            fd(ci, d).wait_recv()
        u = 2 * lt
        left, right = fd_r[0, ci, NS * u], fd_r[1, ci, NS * u]
        far = jnp.where(lane8 < 32, roll(left, -16), roll(right, 16))
        (wa, wb), lse = softweights([lse_c[ci], far])
        wt = jnp.where(lane8 < 64, wa, roll(wb, 64)).T
        for d in range(2):
            m_s[d, ci, half * u] = lse
            for sh in range(half):
                s = d * half + sh
                r = 16 if d == 0 else 48
                ca = wt[r:r + 16, s:s + 1].reshape(1, 2, 8, 1)
                cb = wt[64 + r:80 + r, s:s + 1].reshape(1, 2, 8, 1)
                i = slice(sh * u, (sh + 1) * u)
                a = m_s[d, ci, i].reshape(lt, 2, 8, 128)
                f = fd_r[d, ci, i].reshape(lt, 2, 8, 128)
                m_s[d, ci, i] = (ca * a + cb * f).reshape(u, 8, 128)
            mm(ci, d).start()

    def st_3(ci):
        for d in range(2):
            mm(ci, d).wait_recv()
        u = 2 * lt
        left = roll(jnp.where(row8 < half, m_r[0, ci, half * u], fd_r[0, ci, NS * u]), -16)
        right = roll(jnp.where(row8 < half, fd_r[1, ci, NS * u], m_r[1, ci, half * u]), -48)
        (wo, wl, wr), lse = softweights([lse_c[ci], left, right])
        lse_r[ci] = lse
        for d in range(2):
            fd2_s[d, ci, NS * lt // 2] = lse
        wt = jnp.where(lane8 < 16, wo, jnp.where(lane8 < 32, roll(wl, 16), roll(wr, 32))).T
        res = []
        for s in range(NS):
            hf, sh = s // half, s % half
            im = slice(sh * u, (sh + 1) * u)
            idd = slice((half + sh) * u, (half + sh + 1) * u)
            lv = m_r[0, ci, im] if hf == 0 else fd_r[0, ci, idd]
            rv = fd_r[1, ci, idd] if hf == 0 else m_r[1, ci, im]
            vals = [acc[ci, s * u:(s + 1) * u], lv, rv]
            tot = 0.0
            for n, v in enumerate(vals):
                tot = tot + wt[n * 16:(n + 1) * 16, s:s + 1].reshape(1, 2, 8, 1) * v.reshape(lt, 2, 8, 128)
            res.append(tot.reshape(lt, 16, 128))
        for k in range(half):
            hf, kh = (2 * k) // half, k % (half // 2)
            for slot in range(SIDE):
                v = jnp.concatenate([res[2 * k][:, 4 * slot:4 * slot + 4], res[2 * k + 1][:, 4 * slot:4 * slot + 4]], axis=1)
                i = slice(kh * lt, (kh + 1) * lt)
                idd = slice((half // 2 + kh) * lt, (half // 2 + kh + 1) * lt)
                if slot == 0:
                    acc2[ci, k * lt:(k + 1) * lt] = v
                elif slot == 2:
                    fd2_s[hf, ci, i] = v
                else:
                    d = 0 if slot == 1 else 1
                    if hf == 1 - d:
                        fd2_s[d, ci, idd] = v
                    else:
                        m2_s[d, ci, i] = v
        for d in range(2):
            fd2(ci, d).start()

    def col2(wt, r, s):
        return jnp.concatenate([wt[r:r + 4, s:s + 1], wt[r:r + 4, s + 1:s + 2]], axis=0)[None]

    def st_4(ci):
        for d in range(2):
            fd2(ci, d).wait_recv()
        e = NS * lt // 2
        left, right = fd2_r[0, ci, e], fd2_r[1, ci, e]
        far = jnp.where(lane8 < 8, roll(left, -4), roll(right, 4))
        (wa, wb), lse = softweights([lse_r[ci], far])
        wt = jnp.where(lane8 < 64, wa, roll(wb, 64)).T
        for d in range(2):
            m2_s[d, ci, e // 2] = lse
            for kh in range(half // 2):
                s = d * half + 2 * kh
                r = 4 if d == 0 else 12
                i = slice(kh * lt, (kh + 1) * lt)
                m2_s[d, ci, i] = col2(wt, r, s) * m2_s[d, ci, i] + col2(wt, 64 + r, s) * fd2_r[d, ci, i]
            mm2(ci, d).start()

    def st_5(ci):
        for d in range(2):
            mm2(ci, d).wait_recv()
        e = NS * lt // 2
        left = roll(jnp.where(row8 < half, m2_r[0, ci, e // 2], fd2_r[0, ci, e]), -4)
        right = roll(jnp.where(row8 < half, fd2_r[1, ci, e], m2_r[1, ci, e // 2]), -12)
        (wo, wl, wr), _ = softweights([lse_r[ci], left, right])
        wt = jnp.where(lane8 < 16, wo, jnp.where(lane8 < 32, roll(wl, 16), roll(wr, 32))).T
        for k in range(half):
            hf, kh = (2 * k) // half, k % (half // 2)
            i = slice(kh * lt, (kh + 1) * lt)
            idd = slice((half // 2 + kh) * lt, (half // 2 + kh + 1) * lt)
            lv = m2_r[0, ci, i] if hf == 0 else fd2_r[0, ci, idd]
            rv = fd2_r[1, ci, idd] if hf == 0 else m2_r[1, ci, i]
            s = 2 * k
            tot = col2(wt, 0, s) * acc2[ci, k * lt:(k + 1) * lt] + col2(wt, 16, s) * lv + col2(wt, 32, s) * rv
            b = first(ci) + s
            for n in range(2):
                for l in range(lt):
                    out_ref[b + n, :, l * 128:(l + 1) * 128] = tot[l, 4 * n:4 * n + 4].astype(BF16)

    def send_p1(ci, _):
        for d in range(2):
            p1(ci, d).start()
        return 0

    cols[...] = jnp.zeros_like(cols)
    def each(fn):
        def body(ci, _):
            fn(ci)
            return 0
        lax.fori_loop(0, nc, body, 0)

    lax.fori_loop(0, nc, send_p1, 0)
    each(st_p1f)

    stages = [(LAG_P1R, st_p1r), (LAG_FW, st_fw), (LAG_FR, st_fr), (LAG_C, st_c),
              (LAG_1, st_1), (LAG_2, st_2), (LAG_3, st_3), (LAG_4, st_4), (LAG_5, st_5)]

    def step(i, _):
        for lag, fn in stages:
            ci = i - lag

            @pl.when(jnp.logical_and(ci >= 0, ci < nc))
            def _():
                fn(ci)
        return 0

    lax.fori_loop(0, nc + LAG_5, step, 0)

    def drain(ref, sem):
        pltpu.make_async_copy(ref, ref, sem).wait()

    for d in range(2):
        drain(qraw.at[d], s_p1.at[d])
        drain(qraw.at[d, pl.ds(0, nseq // 2)], s_p1.at[2 + d])
        drain(qm.at[0], s_p2.at[d])
        drain(qm.at[0, :, pl.ds(0, ht)], s_p2.at[2 + d])
        drain(fd_s.at[d], s_fd.at[d])
        drain(m_s.at[d], s_m.at[d])
        drain(fd2_s.at[d], s_fd2.at[d])
        drain(m2_s.at[d], s_m2.at[d])
    for slot in range(SIDE):
        drain(qm.at[slot], s_qp.at[slot])
    drain(o_send, s_o.at[0])
    drain(lse_own, s_o.at[1])


def solution(mesh):
    assert mesh.shape['dcp'] == 2 * SIDE * SIDE

    def local(q, cache, lengths):
        nseq, heads, wd = q.shape
        sl = cache.shape[1]
        lat = wd - ROPE
        lt = lat // 128
        nc = nseq // NS
        nt = NS * lt + NS // 2
        vm = pltpu.VMEM
        dma = pltpu.SemaphoreType.DMA
        scratch = [
            vm((3, nseq, heads, wd), BF16),
            vm((SIDE, nc, nt, 16, 128), BF16),
            vm((SIDE, nc, nt, 16, 128), BF16),
            vm((NB, wd, sl), BF16),
            vm((128, 128), F32),
            vm((nc, NS * SIDE * lt, 16, 128), BF16),
            vm((nc, NS * SIDE * lt, 16, 128), BF16),
            vm((nc, NS * SIDE * lt, 16, 128), BF16),
            vm((nc, 8, 128), F32),
            vm((nc, 8, 128), F32),
            vm((nc, 8, 128), F32),
            vm((nc, 8, 128), F32),
            vm((2, nc, NS * 2 * lt + 1, 8, 128), F32),
            vm((2, nc, NS * 2 * lt + 1, 8, 128), F32),
            vm((2, nc, NS * lt + 1, 8, 128), F32),
            vm((2, nc, NS * lt + 1, 8, 128), F32),
            vm((nc, NS * 2 * lt, 8, 128), F32),
            vm((2, nc, NS * lt // 2 + 1, 8, 128), F32),
            vm((2, nc, NS * lt // 2 + 1, 8, 128), F32),
            vm((2, nc, NS * lt // 4 + 1, 8, 128), F32),
            vm((2, nc, NS * lt // 4 + 1, 8, 128), F32),
            vm((nc, NS * lt // 2, 8, 128), F32),
            dma((NB,)),
            dma((4,)), dma((nc, 4)),
            dma((4,)), dma((nc, 4)),
            dma((4,)), dma((nc, 4)),
            dma((2,)), dma((nc, 2)),
            dma((2,)), dma((nc, 2)),
            dma((2,)), dma((nc, 2)),
            dma((2,)), dma((nc, 2)),
            dma((2,)), dma((nc, 2)),
        ]
        return pl.pallas_call(
            functools.partial(kernel, nc),
            out_shape=jax.ShapeDtypeStruct((nseq, heads, lat), BF16),
            in_specs=[
                pl.BlockSpec(memory_space=pltpu.SMEM),
                pl.BlockSpec(memory_space=pltpu.VMEM),
                pl.BlockSpec(memory_space=pl.ANY),
            ],
            out_specs=pl.BlockSpec(memory_space=pltpu.VMEM),
            scratch_shapes=scratch,
            compiler_params=pltpu.CompilerParams(collective_id=0, has_side_effects=True, vmem_limit_bytes=67_000_000),
        )(lengths, q, jnp.swapaxes(cache, 1, 2))

    return jax.shard_map(local, mesh=mesh, in_specs=(P('dp', 'dcp', None), P('dp', 'dcp', None), P('dp')),
                         out_specs=P('dp', 'dcp', None), check_vma=False)
```

```python
import functools

import jax
import jax.numpy as jnp
from jax import lax
from jax.experimental import pallas as pl
from jax.experimental.pallas import tpu as pltpu
from jax.sharding import PartitionSpec as P

ROPE = 64
SCALE = 192 ** -0.5
SIDE = 4
NS = 4
NB = 8
NEG = float('-inf')
LOG2E = 1.4426950408889634
LN2 = 0.6931471805599453
F32 = jnp.float32
BF16 = jnp.bfloat16

LAG_P1R, LAG_FW, LAG_FR, LAG_C = 0, 5, 10, 11
LAG_1, LAG_2, LAG_3, LAG_4, LAG_5 = 12, 16, 20, 24, 28


def softweights(parts):
    m = functools.reduce(jnp.maximum, parts)
    m0 = jnp.where(m == NEG, 0.0, m)
    ws = [jnp.exp(x - m0) for x in parts]
    tot = functools.reduce(jnp.add, ws)
    inv = 1.0 / jnp.where(tot == 0.0, 1.0, tot)
    return [w * inv for w in ws], m0 + jnp.log(tot)


def roll(x, shift):
    return pltpu.roll(x, shift % 128, 1)


def kernel(nc, len_ref, q_ref, cache_ref, out_ref,
           qraw, qm, qp, cbuf, cols, o_mine, o_send, o_recv, lse_own, lse_recv, lse_c, lse_r,
           fd_s, fd_r, m_s, m_r, acc, fd2_s, fd2_r, m2_s, m2_r, acc2,
           csem, s_p1, r_p1, s_p2, r_p2, s_qp, r_qp, s_o, r_o, s_fd, r_fd, s_m, r_m, s_fd2, r_fd2, s_m2, r_m2):
    me = lax.axis_index('dcp')
    core = me % 2
    x = (me // 2) % SIDE
    y = me // (2 * SIDE)
    nseq = q_ref.shape[0]
    sl = cbuf.shape[2]
    lat = out_ref.shape[2]
    lt = lat // 128
    half = NS // 2
    nt = qm.shape[2]
    ht = nt // 2

    def dev(xx, yy, cc):
        return {'dcp': (((yy + SIDE) % SIDE) * SIDE + (xx + SIDE) % SIDE) * 2 + cc}

    def small(ci, step):
        c = ci % 2
        return dev(x + (1 - c) * step, y + c * step, core)

    def big(ci, step):
        c = ci % 2
        return dev(x + c * step, y + (1 - c) * step, core)

    partner = dev(x, y, 1 - core)

    def first(ci):
        return (ci % 2) * (nseq // 2) + (ci // 2) * NS

    def rcopy(src, dst, ssem, rsem, to):
        return pltpu.make_async_remote_copy(src_ref=src, dst_ref=dst, send_sem=ssem, recv_sem=rsem, device_id=to,
                                            device_id_type=pl.DeviceIdType.MESH)

    def fetch(t):
        ci, s = t // NS, t % NS
        b = first(ci) + s
        return pltpu.make_async_copy(cache_ref.at[b], cbuf.at[t % NB], csem.at[t % NB])

    for t in range(NB):
        fetch(t).start()

    barrier = pltpu.get_barrier_semaphore()
    for to in (dev(x + 1, y, core), dev(x - 1, y, core), dev(x, y + 1, core), dev(x, y - 1, core), partner):
        pl.semaphore_signal(barrier, inc=1, device_id=to, device_id_type=pl.DeviceIdType.MESH)
    pl.semaphore_wait(barrier, 5)

    def p1(ci, d):
        sq = pl.ds(first(ci), NS)
        return rcopy(q_ref.at[sq], qraw.at[d, sq], s_p1.at[d], r_p1.at[ci, d], small(ci, 1 - 2 * d))

    def p1f(ci, d):
        sq = pl.ds(first(ci) + d * half, half)
        return rcopy(qraw.at[d, sq], qraw.at[2, sq], s_p1.at[2 + d], r_p1.at[ci, 2 + d], small(ci, 1 - 2 * d))

    def p2(ci, d):
        return rcopy(qm.at[0, ci], qm.at[3 - 2 * d, ci], s_p2.at[d], r_p2.at[ci, d], big(ci, 1 - 2 * d))

    def p2f(ci, d):
        tl = pl.ds(d * ht, ht)
        return rcopy(qm.at[3 - 2 * d, ci, tl], qm.at[2, ci, tl], s_p2.at[2 + d], r_p2.at[ci, 2 + d], big(ci, 1 - 2 * d))

    def toq(ci, slot):
        return rcopy(qm.at[slot, ci], qp.at[slot, ci], s_qp.at[slot], r_qp.at[ci, slot], partner)

    def too(ci):
        return rcopy(o_send.at[ci], o_recv.at[ci], s_o.at[0], r_o.at[ci, 0], partner)

    def tol(ci):
        return rcopy(lse_own.at[ci], lse_recv.at[ci], s_o.at[1], r_o.at[ci, 1], partner)

    def fd(ci, d):
        return rcopy(fd_s.at[d, ci], fd_r.at[d, ci], s_fd.at[d], r_fd.at[ci, d], big(ci, 1 - 2 * d))

    def mm(ci, d):
        return rcopy(m_s.at[d, ci], m_r.at[d, ci], s_m.at[d], r_m.at[ci, d], big(ci, 1 - 2 * d))

    def fd2(ci, d):
        return rcopy(fd2_s.at[d, ci], fd2_r.at[d, ci], s_fd2.at[d], r_fd2.at[ci, d], small(ci, 1 - 2 * d))

    def mm2(ci, d):
        return rcopy(m2_s.at[d, ci], m2_r.at[d, ci], s_m2.at[d], r_m2.at[ci, d], small(ci, 1 - 2 * d))

    def st_p1f(ci):
        for d in range(2):
            p1(ci, d).wait_recv()
            p1f(ci, d).start()

    def st_p1r(ci):
        for d in range(2):
            p1f(ci, d).wait_recv()
        ropes = []
        for s in range(NS):
            b = first(ci) + s
            rows = [q_ref[b], qraw[1, b], qraw[2, b], qraw[0, b]]
            rows = jnp.concatenate([r.astype(F32) for r in rows], axis=0)
            for l in range(lt):
                qm[0, ci, s * lt + l] = rows[:, l * 128:(l + 1) * 128].astype(BF16)
            ropes.append(rows[:, lat:lat + ROPE])
            if s % 2:
                qm[0, ci, NS * lt + s // 2] = jnp.concatenate(ropes[s - 1:s + 1], axis=1).astype(BF16)
        for d in range(2):
            p2(ci, d).start()
        toq(ci, 0).start()

    def st_fw(ci):
        for d in range(2):
            p2(ci, d).wait_recv()
            p2f(ci, d).start()
        toq(ci, 3).start()
        toq(ci, 1).start()

    def st_fr(ci):
        for d in range(2):
            p2f(ci, d).wait_recv()
        toq(ci, 2).start()

    lane128 = lax.broadcasted_iota(jnp.int32, (128, 128), 1)

    def st_c(ci):
        for slot in range(SIDE):
            toq(ci, slot).wait_recv()

        for s in range(NS):
            fetch(ci * NS + s).wait()

        def block(s):
            return cbuf.at[(ci * NS + s) % NB]

        def scores(s):
            idx = [s * lt + l for l in range(lt)] + [NS * lt + s // 2]
            tiles = [jnp.concatenate([qm[:, ci, i].reshape(64, 128), qp[:, ci, i].reshape(64, 128)], axis=0) for i in idx]
            tiles[lt] = tiles[lt][:, s % 2 * ROPE:(s % 2 + 1) * ROPE]
            q = jnp.concatenate(tiles, axis=1)
            return lax.dot_general(q, block(s)[...], (((1,), (0,)), ((), ())), preferred_element_type=F32)

        def attend(s, sc):
            sc = jnp.where(pos < len_ref[first(ci) + s], sc * (SCALE * LOG2E), NEG)
            m = jnp.max(sc, axis=1, keepdims=True)
            m0 = jnp.where(m == NEG, 0.0, m)
            p = jnp.exp2(sc - m0)
            ls = jnp.sum(p, axis=1, keepdims=True)
            pv = lax.dot_general(p.astype(BF16), block(s)[:lat], (((1,), (1,)), ((), ())), preferred_element_type=F32)
            l1 = jnp.where(ls > 0.0, ls, 1.0)
            o = (pv * (1.0 / l1)).astype(BF16)
            for slot in range(2 * SIDE):
                to = o_mine if slot < SIDE else o_send
                for l in range(lt):
                    to[ci, (s * SIDE + slot % SIDE) * lt + l] = o[slot * 16:(slot + 1) * 16, l * 128:(l + 1) * 128]
            return m0 * LN2 + jnp.log(ls)

        pos = me * sl + lax.broadcasted_iota(jnp.int32, (1, sl), 1)
        sc = scores(0)
        for s in range(NS):
            after = scores(s + 1) if s + 1 < NS else None
            lse = attend(s, sc)
            cols[...] = jnp.where(lane128 == s, lse, cols[...])
            sc = after

        for s in range(NS):
            t = (ci + NB // NS) * NS + s

            @pl.when(t < nc * NS)
            def _():
                fetch(t).start()

        lse_own[ci] = cols[...].T[:8]
        too(ci).start()
        tol(ci).start()

    row8 = lax.broadcasted_iota(jnp.int32, (8, 128), 0)
    lane8 = lax.broadcasted_iota(jnp.int32, (8, 128), 1)

    def st_1(ci):
        too(ci).wait_recv()
        tol(ci).wait_recv()
        own = lse_own[ci]
        (wa, wb), lse = softweights([own, roll(lse_recv[ci], 64)])
        lse_c[ci] = lse
        wt = jnp.where(lane8 < 64, wa, roll(wb, 64)).T
        for d in range(2):
            fd_s[d, ci, NS * 2 * lt] = lse
        u = 2 * lt
        for s in range(NS):
            hf, sh = s // half, s % half
            for slot in range(SIDE):
                i = pl.ds((s * SIDE + slot) * lt, lt)
                ca = wt[slot * 16:(slot + 1) * 16, s:s + 1][None]
                cb = wt[64 + slot * 16:64 + (slot + 1) * 16, s:s + 1][None]
                v = (ca * o_mine[ci, i].astype(F32) + cb * o_recv[ci, i].astype(F32)).reshape(u, 8, 128)
                if slot == 0:
                    acc[ci, s * u:(s + 1) * u] = v
                elif slot == 2:
                    fd_s[hf, ci, sh * u:(sh + 1) * u] = v
                else:
                    d = 0 if slot == 1 else 1
                    if hf == 1 - d:
                        fd_s[d, ci, (half + sh) * u:(half + sh + 1) * u] = v
                    else:
                        m_s[d, ci, sh * u:(sh + 1) * u] = v
        for d in range(2):
            fd(ci, d).start()

    def st_2(ci):
        for d in range(2):
            fd(ci, d).wait_recv()
        u = 2 * lt
        left, right = fd_r[0, ci, NS * u], fd_r[1, ci, NS * u]
        far = jnp.where(lane8 < 32, roll(left, -16), roll(right, 16))
        (wa, wb), lse = softweights([lse_c[ci], far])
        wt = jnp.where(lane8 < 64, wa, roll(wb, 64)).T
        for d in range(2):
            m_s[d, ci, half * u] = lse
            for sh in range(half):
                s = d * half + sh
                r = 16 if d == 0 else 48
                ca = wt[r:r + 16, s:s + 1].reshape(1, 2, 8, 1)
                cb = wt[64 + r:80 + r, s:s + 1].reshape(1, 2, 8, 1)
                i = slice(sh * u, (sh + 1) * u)
                a = m_s[d, ci, i].reshape(lt, 2, 8, 128)
                f = fd_r[d, ci, i].reshape(lt, 2, 8, 128)
                m_s[d, ci, i] = (ca * a + cb * f).reshape(u, 8, 128)
            mm(ci, d).start()

    def st_3(ci):
        for d in range(2):
            mm(ci, d).wait_recv()
        u = 2 * lt
        left = roll(jnp.where(row8 < half, m_r[0, ci, half * u], fd_r[0, ci, NS * u]), -16)
        right = roll(jnp.where(row8 < half, fd_r[1, ci, NS * u], m_r[1, ci, half * u]), -48)
        (wo, wl, wr), lse = softweights([lse_c[ci], left, right])
        lse_r[ci] = lse
        for d in range(2):
            fd2_s[d, ci, NS * lt // 2] = lse
        wt = jnp.where(lane8 < 16, wo, jnp.where(lane8 < 32, roll(wl, 16), roll(wr, 32))).T
        res = []
        for s in range(NS):
            hf, sh = s // half, s % half
            im = slice(sh * u, (sh + 1) * u)
            idd = slice((half + sh) * u, (half + sh + 1) * u)
            lv = m_r[0, ci, im] if hf == 0 else fd_r[0, ci, idd]
            rv = fd_r[1, ci, idd] if hf == 0 else m_r[1, ci, im]
            vals = [acc[ci, s * u:(s + 1) * u], lv, rv]
            tot = 0.0
            for n, v in enumerate(vals):
                tot = tot + wt[n * 16:(n + 1) * 16, s:s + 1].reshape(1, 2, 8, 1) * v.reshape(lt, 2, 8, 128)
            res.append(tot.reshape(lt, 16, 128))
        for k in range(half):
            hf, kh = (2 * k) // half, k % (half // 2)
            for slot in range(SIDE):
                v = jnp.concatenate([res[2 * k][:, 4 * slot:4 * slot + 4], res[2 * k + 1][:, 4 * slot:4 * slot + 4]], axis=1)
                i = slice(kh * lt, (kh + 1) * lt)
                idd = slice((half // 2 + kh) * lt, (half // 2 + kh + 1) * lt)
                if slot == 0:
                    acc2[ci, k * lt:(k + 1) * lt] = v
                elif slot == 2:
                    fd2_s[hf, ci, i] = v
                else:
                    d = 0 if slot == 1 else 1
                    if hf == 1 - d:
                        fd2_s[d, ci, idd] = v
                    else:
                        m2_s[d, ci, i] = v
        for d in range(2):
            fd2(ci, d).start()

    def col2(wt, r, s):
        return jnp.concatenate([wt[r:r + 4, s:s + 1], wt[r:r + 4, s + 1:s + 2]], axis=0)[None]

    def st_4(ci):
        for d in range(2):
            fd2(ci, d).wait_recv()
        e = NS * lt // 2
        left, right = fd2_r[0, ci, e], fd2_r[1, ci, e]
        far = jnp.where(lane8 < 8, roll(left, -4), roll(right, 4))
        (wa, wb), lse = softweights([lse_r[ci], far])
        wt = jnp.where(lane8 < 64, wa, roll(wb, 64)).T
        for d in range(2):
            m2_s[d, ci, e // 2] = lse
            for kh in range(half // 2):
                s = d * half + 2 * kh
                r = 4 if d == 0 else 12
                i = slice(kh * lt, (kh + 1) * lt)
                m2_s[d, ci, i] = col2(wt, r, s) * m2_s[d, ci, i] + col2(wt, 64 + r, s) * fd2_r[d, ci, i]
            mm2(ci, d).start()

    def st_5(ci):
        for d in range(2):
            mm2(ci, d).wait_recv()
        e = NS * lt // 2
        left = roll(jnp.where(row8 < half, m2_r[0, ci, e // 2], fd2_r[0, ci, e]), -4)
        right = roll(jnp.where(row8 < half, fd2_r[1, ci, e], m2_r[1, ci, e // 2]), -12)
        (wo, wl, wr), _ = softweights([lse_r[ci], left, right])
        wt = jnp.where(lane8 < 16, wo, jnp.where(lane8 < 32, roll(wl, 16), roll(wr, 32))).T
        for k in range(half):
            hf, kh = (2 * k) // half, k % (half // 2)
            i = slice(kh * lt, (kh + 1) * lt)
            idd = slice((half // 2 + kh) * lt, (half // 2 + kh + 1) * lt)
            lv = m2_r[0, ci, i] if hf == 0 else fd2_r[0, ci, idd]
            rv = fd2_r[1, ci, idd] if hf == 0 else m2_r[1, ci, i]
            s = 2 * k
            tot = col2(wt, 0, s) * acc2[ci, k * lt:(k + 1) * lt] + col2(wt, 16, s) * lv + col2(wt, 32, s) * rv
            b = first(ci) + s
            for n in range(2):
                for l in range(lt):
                    out_ref[b + n, :, l * 128:(l + 1) * 128] = tot[l, 4 * n:4 * n + 4].astype(BF16)

    def send_p1(ci, _):
        for d in range(2):
            p1(ci, d).start()
        return 0

    cols[...] = jnp.zeros_like(cols)
    def each(fn):
        def body(ci, _):
            fn(ci)
            return 0
        lax.fori_loop(0, nc, body, 0)

    lax.fori_loop(0, nc, send_p1, 0)
    each(st_p1f)

    stages = [(LAG_P1R, st_p1r), (LAG_FW, st_fw), (LAG_FR, st_fr), (LAG_C, st_c),
              (LAG_1, st_1), (LAG_2, st_2), (LAG_3, st_3), (LAG_4, st_4), (LAG_5, st_5)]

    def step(i, _):
        for lag, fn in stages:
            ci = i - lag

            @pl.when(jnp.logical_and(ci >= 0, ci < nc))
            def _():
                fn(ci)
        return 0

    lax.fori_loop(0, nc + LAG_5, step, 0)

    def drain(ref, sem):
        pltpu.make_async_copy(ref, ref, sem).wait()

    for d in range(2):
        drain(qraw.at[d], s_p1.at[d])
        drain(qraw.at[d, pl.ds(0, nseq // 2)], s_p1.at[2 + d])
        drain(qm.at[0], s_p2.at[d])
        drain(qm.at[0, :, pl.ds(0, ht)], s_p2.at[2 + d])
        drain(fd_s.at[d], s_fd.at[d])
        drain(m_s.at[d], s_m.at[d])
        drain(fd2_s.at[d], s_fd2.at[d])
        drain(m2_s.at[d], s_m2.at[d])
    for slot in range(SIDE):
        drain(qm.at[slot], s_qp.at[slot])
    drain(o_send, s_o.at[0])
    drain(lse_own, s_o.at[1])


def solution(mesh):
    assert mesh.shape['dcp'] == 2 * SIDE * SIDE

    def local(q, cache, lengths):
        nseq, heads, wd = q.shape
        sl = cache.shape[1]
        lat = wd - ROPE
        lt = lat // 128
        nc = nseq // NS
        nt = NS * lt + NS // 2
        vm = pltpu.VMEM
        dma = pltpu.SemaphoreType.DMA
        scratch = [
            vm((3, nseq, heads, wd), BF16),
            vm((SIDE, nc, nt, 16, 128), BF16),
            vm((SIDE, nc, nt, 16, 128), BF16),
            vm((NB, wd, sl), BF16),
            vm((128, 128), F32),
            vm((nc, NS * SIDE * lt, 16, 128), BF16),
            vm((nc, NS * SIDE * lt, 16, 128), BF16),
            vm((nc, NS * SIDE * lt, 16, 128), BF16),
            vm((nc, 8, 128), F32),
            vm((nc, 8, 128), F32),
            vm((nc, 8, 128), F32),
            vm((nc, 8, 128), F32),
            vm((2, nc, NS * 2 * lt + 1, 8, 128), F32),
            vm((2, nc, NS * 2 * lt + 1, 8, 128), F32),
            vm((2, nc, NS * lt + 1, 8, 128), F32),
            vm((2, nc, NS * lt + 1, 8, 128), F32),
            vm((nc, NS * 2 * lt, 8, 128), F32),
            vm((2, nc, NS * lt // 2 + 1, 8, 128), F32),
            vm((2, nc, NS * lt // 2 + 1, 8, 128), F32),
            vm((2, nc, NS * lt // 4 + 1, 8, 128), F32),
            vm((2, nc, NS * lt // 4 + 1, 8, 128), F32),
            vm((nc, NS * lt // 2, 8, 128), F32),
            dma((NB,)),
            dma((4,)), dma((nc, 4)),
            dma((4,)), dma((nc, 4)),
            dma((4,)), dma((nc, 4)),
            dma((2,)), dma((nc, 2)),
            dma((2,)), dma((nc, 2)),
            dma((2,)), dma((nc, 2)),
            dma((2,)), dma((nc, 2)),
            dma((2,)), dma((nc, 2)),
        ]
        return pl.pallas_call(
            functools.partial(kernel, nc),
            out_shape=jax.ShapeDtypeStruct((nseq, heads, lat), BF16),
            in_specs=[
                pl.BlockSpec(memory_space=pltpu.SMEM),
                pl.BlockSpec(memory_space=pltpu.VMEM),
                pl.BlockSpec(memory_space=pl.ANY),
            ],
            out_specs=pl.BlockSpec(memory_space=pltpu.VMEM),
            scratch_shapes=scratch,
            compiler_params=pltpu.CompilerParams(collective_id=0, has_side_effects=True, vmem_limit_bytes=67_000_000),
        )(lengths, q, jnp.swapaxes(cache, 1, 2))

    return jax.shard_map(local, mesh=mesh, in_specs=(P('dp', 'dcp', None), P('dp', 'dcp', None), P('dp')),
                         out_specs=P('dp', 'dcp', None), check_vma=False)
```

```python
import functools

import jax
import jax.numpy as jnp
from jax import lax
from jax.experimental import pallas as pl
from jax.experimental.pallas import tpu as pltpu
from jax.sharding import PartitionSpec as P

ROPE = 64
SCALE = 192 ** -0.5
SIDE = 4
NS = 4
NB = 8
NEG = float('-inf')
LOG2E = 1.4426950408889634
LN2 = 0.6931471805599453
F32 = jnp.float32
BF16 = jnp.bfloat16

LAG_P1R, LAG_FW, LAG_FR, LAG_C = 0, 5, 10, 11
LAG_1, LAG_2, LAG_3, LAG_4, LAG_5 = 12, 16, 20, 24, 28


def softweights(parts):
    m = functools.reduce(jnp.maximum, parts)
    m0 = jnp.where(m == NEG, 0.0, m)
    ws = [jnp.exp(x - m0) for x in parts]
    tot = functools.reduce(jnp.add, ws)
    inv = 1.0 / jnp.where(tot == 0.0, 1.0, tot)
    return [w * inv for w in ws], m0 + jnp.log(tot)


def roll(x, shift):
    return pltpu.roll(x, shift % 128, 1)


def kernel(nc, len_ref, q_hbm, cache_ref, out_ref,
           q_ref, qsem, qraw, qm, qp, cbuf, cols, o_mine, o_send, o_recv, lse_own, lse_recv, lse_c, lse_r,
           fd_s, fd_r, m_s, m_r, acc, fd2_s, fd2_r, m2_s, m2_r, acc2,
           csem, s_p1, r_p1, s_p2, r_p2, s_qp, r_qp, s_o, r_o, s_fd, r_fd, s_m, r_m, s_fd2, r_fd2, s_m2, r_m2):
    me = lax.axis_index('dcp')
    core = me % 2
    x = (me // 2) % SIDE
    y = me // (2 * SIDE)
    nseq = q_ref.shape[0]
    sl = cbuf.shape[2]
    lat = out_ref.shape[2]
    lt = lat // 128
    half = NS // 2
    nt = qm.shape[2]
    ht = nt // 2

    def dev(xx, yy, cc):
        return {'dcp': (((yy + SIDE) % SIDE) * SIDE + (xx + SIDE) % SIDE) * 2 + cc}

    def small(ci, step):
        c = ci % 2
        return dev(x + (1 - c) * step, y + c * step, core)

    def big(ci, step):
        c = ci % 2
        return dev(x + c * step, y + (1 - c) * step, core)

    partner = dev(x, y, 1 - core)

    def first(ci):
        return (ci % 2) * (nseq // 2) + (ci // 2) * NS

    def rcopy(src, dst, ssem, rsem, to):
        return pltpu.make_async_remote_copy(src_ref=src, dst_ref=dst, send_sem=ssem, recv_sem=rsem, device_id=to,
                                            device_id_type=pl.DeviceIdType.MESH)

    def fetch(t):
        ci, s = t // NS, t % NS
        b = first(ci) + s
        return pltpu.make_async_copy(cache_ref.at[b], cbuf.at[t % NB], csem.at[t % NB])

    barrier = pltpu.get_barrier_semaphore()
    for to in (dev(x + 1, y, core), dev(x - 1, y, core), dev(x, y + 1, core), dev(x, y - 1, core), partner):
        pl.semaphore_signal(barrier, inc=1, device_id=to, device_id_type=pl.DeviceIdType.MESH)
    own = pltpu.make_async_copy(q_hbm, q_ref, qsem)
    own.start()
    for t in range(NB):
        fetch(t).start()
    own.wait()
    pl.semaphore_wait(barrier, 5)

    def p1(ci, d):
        sq = pl.ds(first(ci), NS)
        return rcopy(q_ref.at[sq], qraw.at[d, sq], s_p1.at[d], r_p1.at[ci, d], small(ci, 1 - 2 * d))

    def p1f(ci, d):
        sq = pl.ds(first(ci) + d * half, half)
        return rcopy(qraw.at[d, sq], qraw.at[2, sq], s_p1.at[2 + d], r_p1.at[ci, 2 + d], small(ci, 1 - 2 * d))

    def p2(ci, d):
        return rcopy(qm.at[0, ci], qm.at[3 - 2 * d, ci], s_p2.at[d], r_p2.at[ci, d], big(ci, 1 - 2 * d))

    def p2f(ci, d):
        tl = pl.ds(d * ht, ht)
        return rcopy(qm.at[3 - 2 * d, ci, tl], qm.at[2, ci, tl], s_p2.at[2 + d], r_p2.at[ci, 2 + d], big(ci, 1 - 2 * d))

    def toq(ci, slot):
        return rcopy(qm.at[slot, ci], qp.at[slot, ci], s_qp.at[slot], r_qp.at[ci, slot], partner)

    def too(ci):
        return rcopy(o_send.at[ci], o_recv.at[ci], s_o.at[0], r_o.at[ci, 0], partner)

    def tol(ci):
        return rcopy(lse_own.at[ci], lse_recv.at[ci], s_o.at[1], r_o.at[ci, 1], partner)

    def fd(ci, d):
        return rcopy(fd_s.at[d, ci], fd_r.at[d, ci], s_fd.at[d], r_fd.at[ci, d], big(ci, 1 - 2 * d))

    def mm(ci, d):
        return rcopy(m_s.at[d, ci], m_r.at[d, ci], s_m.at[d], r_m.at[ci, d], big(ci, 1 - 2 * d))

    def fd2(ci, d):
        return rcopy(fd2_s.at[d, ci], fd2_r.at[d, ci], s_fd2.at[d], r_fd2.at[ci, d], small(ci, 1 - 2 * d))

    def mm2(ci, d):
        return rcopy(m2_s.at[d, ci], m2_r.at[d, ci], s_m2.at[d], r_m2.at[ci, d], small(ci, 1 - 2 * d))

    def st_p1f(ci):
        for d in range(2):
            p1(ci, d).wait_recv()
            p1f(ci, d).start()

    def st_p1r(ci):
        for d in range(2):
            p1f(ci, d).wait_recv()
        ropes = []
        for s in range(NS):
            b = first(ci) + s
            rows = [q_ref[b], qraw[1, b], qraw[2, b], qraw[0, b]]
            rows = jnp.concatenate([r.astype(F32) for r in rows], axis=0)
            for l in range(lt):
                qm[0, ci, s * lt + l] = rows[:, l * 128:(l + 1) * 128].astype(BF16)
            ropes.append(rows[:, lat:lat + ROPE])
            if s % 2:
                qm[0, ci, NS * lt + s // 2] = jnp.concatenate(ropes[s - 1:s + 1], axis=1).astype(BF16)
        for d in range(2):
            p2(ci, d).start()
        toq(ci, 0).start()

    def st_fw(ci):
        for d in range(2):
            p2(ci, d).wait_recv()
            p2f(ci, d).start()
        toq(ci, 3).start()
        toq(ci, 1).start()

    def st_fr(ci):
        for d in range(2):
            p2f(ci, d).wait_recv()
        toq(ci, 2).start()

    lane128 = lax.broadcasted_iota(jnp.int32, (128, 128), 1)

    def st_c(ci):
        for slot in range(SIDE):
            toq(ci, slot).wait_recv()

        for s in range(NS):
            fetch(ci * NS + s).wait()

        def block(s):
            return cbuf.at[(ci * NS + s) % NB]

        def scores(s):
            idx = [s * lt + l for l in range(lt)] + [NS * lt + s // 2]
            tiles = [jnp.concatenate([qm[:, ci, i].reshape(64, 128), qp[:, ci, i].reshape(64, 128)], axis=0) for i in idx]
            tiles[lt] = tiles[lt][:, s % 2 * ROPE:(s % 2 + 1) * ROPE]
            q = jnp.concatenate(tiles, axis=1)
            return lax.dot_general(q, block(s)[...], (((1,), (0,)), ((), ())), preferred_element_type=F32)

        def attend(s, sc):
            sc = jnp.where(pos < len_ref[first(ci) + s], sc * (SCALE * LOG2E), NEG)
            m = jnp.max(sc, axis=1, keepdims=True)
            m0 = jnp.where(m == NEG, 0.0, m)
            p = jnp.exp2(sc - m0)
            ls = jnp.sum(p, axis=1, keepdims=True)
            pv = lax.dot_general(p.astype(BF16), block(s)[:lat], (((1,), (1,)), ((), ())), preferred_element_type=F32)
            l1 = jnp.where(ls > 0.0, ls, 1.0)
            o = (pv * (1.0 / l1)).astype(BF16)
            for slot in range(2 * SIDE):
                to = o_mine if slot < SIDE else o_send
                for l in range(lt):
                    to[ci, (s * SIDE + slot % SIDE) * lt + l] = o[slot * 16:(slot + 1) * 16, l * 128:(l + 1) * 128]
            return m0 * LN2 + jnp.log(ls)

        pos = me * sl + lax.broadcasted_iota(jnp.int32, (1, sl), 1)
        sc = scores(0)
        for s in range(NS):
            after = scores(s + 1) if s + 1 < NS else None
            lse = attend(s, sc)
            cols[...] = jnp.where(lane128 == s, lse, cols[...])
            sc = after

        for s in range(NS):
            t = (ci + NB // NS) * NS + s

            @pl.when(t < nc * NS)
            def _():
                fetch(t).start()

        lse_own[ci] = cols[...].T[:8]
        too(ci).start()
        tol(ci).start()

    row8 = lax.broadcasted_iota(jnp.int32, (8, 128), 0)
    lane8 = lax.broadcasted_iota(jnp.int32, (8, 128), 1)

    def st_1(ci):
        too(ci).wait_recv()
        tol(ci).wait_recv()
        own = lse_own[ci]
        (wa, wb), lse = softweights([own, roll(lse_recv[ci], 64)])
        lse_c[ci] = lse
        wt = jnp.where(lane8 < 64, wa, roll(wb, 64)).T
        for d in range(2):
            fd_s[d, ci, NS * 2 * lt] = lse
        u = 2 * lt
        for s in range(NS):
            hf, sh = s // half, s % half
            for slot in range(SIDE):
                i = pl.ds((s * SIDE + slot) * lt, lt)
                ca = wt[slot * 16:(slot + 1) * 16, s:s + 1][None]
                cb = wt[64 + slot * 16:64 + (slot + 1) * 16, s:s + 1][None]
                v = (ca * o_mine[ci, i].astype(F32) + cb * o_recv[ci, i].astype(F32)).reshape(u, 8, 128)
                if slot == 0:
                    acc[ci, s * u:(s + 1) * u] = v
                elif slot == 2:
                    fd_s[hf, ci, sh * u:(sh + 1) * u] = v
                else:
                    d = 0 if slot == 1 else 1
                    if hf == 1 - d:
                        fd_s[d, ci, (half + sh) * u:(half + sh + 1) * u] = v
                    else:
                        m_s[d, ci, sh * u:(sh + 1) * u] = v
        for d in range(2):
            fd(ci, d).start()

    def st_2(ci):
        for d in range(2):
            fd(ci, d).wait_recv()
        u = 2 * lt
        left, right = fd_r[0, ci, NS * u], fd_r[1, ci, NS * u]
        far = jnp.where(lane8 < 32, roll(left, -16), roll(right, 16))
        (wa, wb), lse = softweights([lse_c[ci], far])
        wt = jnp.where(lane8 < 64, wa, roll(wb, 64)).T
        for d in range(2):
            m_s[d, ci, half * u] = lse
            for sh in range(half):
                s = d * half + sh
                r = 16 if d == 0 else 48
                ca = wt[r:r + 16, s:s + 1].reshape(1, 2, 8, 1)
                cb = wt[64 + r:80 + r, s:s + 1].reshape(1, 2, 8, 1)
                i = slice(sh * u, (sh + 1) * u)
                a = m_s[d, ci, i].reshape(lt, 2, 8, 128)
                f = fd_r[d, ci, i].reshape(lt, 2, 8, 128)
                m_s[d, ci, i] = (ca * a + cb * f).reshape(u, 8, 128)
            mm(ci, d).start()

    def st_3(ci):
        for d in range(2):
            mm(ci, d).wait_recv()
        u = 2 * lt
        left = roll(jnp.where(row8 < half, m_r[0, ci, half * u], fd_r[0, ci, NS * u]), -16)
        right = roll(jnp.where(row8 < half, fd_r[1, ci, NS * u], m_r[1, ci, half * u]), -48)
        (wo, wl, wr), lse = softweights([lse_c[ci], left, right])
        lse_r[ci] = lse
        for d in range(2):
            fd2_s[d, ci, NS * lt // 2] = lse
        wt = jnp.where(lane8 < 16, wo, jnp.where(lane8 < 32, roll(wl, 16), roll(wr, 32))).T
        res = []
        for s in range(NS):
            hf, sh = s // half, s % half
            im = slice(sh * u, (sh + 1) * u)
            idd = slice((half + sh) * u, (half + sh + 1) * u)
            lv = m_r[0, ci, im] if hf == 0 else fd_r[0, ci, idd]
            rv = fd_r[1, ci, idd] if hf == 0 else m_r[1, ci, im]
            vals = [acc[ci, s * u:(s + 1) * u], lv, rv]
            tot = 0.0
            for n, v in enumerate(vals):
                tot = tot + wt[n * 16:(n + 1) * 16, s:s + 1].reshape(1, 2, 8, 1) * v.reshape(lt, 2, 8, 128)
            res.append(tot.reshape(lt, 16, 128))
        for k in range(half):
            hf, kh = (2 * k) // half, k % (half // 2)
            for slot in range(SIDE):
                v = jnp.concatenate([res[2 * k][:, 4 * slot:4 * slot + 4], res[2 * k + 1][:, 4 * slot:4 * slot + 4]], axis=1)
                i = slice(kh * lt, (kh + 1) * lt)
                idd = slice((half // 2 + kh) * lt, (half // 2 + kh + 1) * lt)
                if slot == 0:
                    acc2[ci, k * lt:(k + 1) * lt] = v
                elif slot == 2:
                    fd2_s[hf, ci, i] = v
                else:
                    d = 0 if slot == 1 else 1
                    if hf == 1 - d:
                        fd2_s[d, ci, idd] = v
                    else:
                        m2_s[d, ci, i] = v
        for d in range(2):
            fd2(ci, d).start()

    def col2(wt, r, s):
        return jnp.concatenate([wt[r:r + 4, s:s + 1], wt[r:r + 4, s + 1:s + 2]], axis=0)[None]

    def st_4(ci):
        for d in range(2):
            fd2(ci, d).wait_recv()
        e = NS * lt // 2
        left, right = fd2_r[0, ci, e], fd2_r[1, ci, e]
        far = jnp.where(lane8 < 8, roll(left, -4), roll(right, 4))
        (wa, wb), lse = softweights([lse_r[ci], far])
        wt = jnp.where(lane8 < 64, wa, roll(wb, 64)).T
        for d in range(2):
            m2_s[d, ci, e // 2] = lse
            for kh in range(half // 2):
                s = d * half + 2 * kh
                r = 4 if d == 0 else 12
                i = slice(kh * lt, (kh + 1) * lt)
                m2_s[d, ci, i] = col2(wt, r, s) * m2_s[d, ci, i] + col2(wt, 64 + r, s) * fd2_r[d, ci, i]
            mm2(ci, d).start()

    def st_5(ci):
        for d in range(2):
            mm2(ci, d).wait_recv()
        e = NS * lt // 2
        left = roll(jnp.where(row8 < half, m2_r[0, ci, e // 2], fd2_r[0, ci, e]), -4)
        right = roll(jnp.where(row8 < half, fd2_r[1, ci, e], m2_r[1, ci, e // 2]), -12)
        (wo, wl, wr), _ = softweights([lse_r[ci], left, right])
        wt = jnp.where(lane8 < 16, wo, jnp.where(lane8 < 32, roll(wl, 16), roll(wr, 32))).T
        for k in range(half):
            hf, kh = (2 * k) // half, k % (half // 2)
            i = slice(kh * lt, (kh + 1) * lt)
            idd = slice((half // 2 + kh) * lt, (half // 2 + kh + 1) * lt)
            lv = m2_r[0, ci, i] if hf == 0 else fd2_r[0, ci, idd]
            rv = fd2_r[1, ci, idd] if hf == 0 else m2_r[1, ci, i]
            s = 2 * k
            tot = col2(wt, 0, s) * acc2[ci, k * lt:(k + 1) * lt] + col2(wt, 16, s) * lv + col2(wt, 32, s) * rv
            b = first(ci) + s
            for n in range(2):
                for l in range(lt):
                    out_ref[b + n, :, l * 128:(l + 1) * 128] = tot[l, 4 * n:4 * n + 4].astype(BF16)

    def send_p1(ci, _):
        for d in range(2):
            p1(ci, d).start()
        return 0

    cols[...] = jnp.zeros_like(cols)
    def each(fn):
        def body(ci, _):
            fn(ci)
            return 0
        lax.fori_loop(0, nc, body, 0)

    lax.fori_loop(0, nc, send_p1, 0)
    each(st_p1f)

    stages = [(LAG_P1R, st_p1r), (LAG_FW, st_fw), (LAG_FR, st_fr), (LAG_C, st_c),
              (LAG_1, st_1), (LAG_2, st_2), (LAG_3, st_3), (LAG_4, st_4), (LAG_5, st_5)]

    def step(i, _):
        for lag, fn in stages:
            ci = i - lag

            @pl.when(jnp.logical_and(ci >= 0, ci < nc))
            def _():
                fn(ci)
        return 0

    lax.fori_loop(0, nc + LAG_5, step, 0)

    def drain(ref, sem):
        pltpu.make_async_copy(ref, ref, sem).wait()

    for d in range(2):
        drain(qraw.at[d], s_p1.at[d])
        drain(qraw.at[d, pl.ds(0, nseq // 2)], s_p1.at[2 + d])
        drain(qm.at[0], s_p2.at[d])
        drain(qm.at[0, :, pl.ds(0, ht)], s_p2.at[2 + d])
        drain(fd_s.at[d], s_fd.at[d])
        drain(m_s.at[d], s_m.at[d])
        drain(fd2_s.at[d], s_fd2.at[d])
        drain(m2_s.at[d], s_m2.at[d])
    for slot in range(SIDE):
        drain(qm.at[slot], s_qp.at[slot])
    drain(o_send, s_o.at[0])
    drain(lse_own, s_o.at[1])


def solution(mesh):
    assert mesh.shape['dcp'] == 2 * SIDE * SIDE

    def local(q, cache, lengths):
        nseq, heads, wd = q.shape
        sl = cache.shape[1]
        lat = wd - ROPE
        lt = lat // 128
        nc = nseq // NS
        nt = NS * lt + NS // 2
        vm = pltpu.VMEM
        dma = pltpu.SemaphoreType.DMA
        scratch = [
            vm((nseq, heads, wd), BF16),
            dma(()),
            vm((3, nseq, heads, wd), BF16),
            vm((SIDE, nc, nt, 16, 128), BF16),
            vm((SIDE, nc, nt, 16, 128), BF16),
            vm((NB, wd, sl), BF16),
            vm((128, 128), F32),
            vm((nc, NS * SIDE * lt, 16, 128), BF16),
            vm((nc, NS * SIDE * lt, 16, 128), BF16),
            vm((nc, NS * SIDE * lt, 16, 128), BF16),
            vm((nc, 8, 128), F32),
            vm((nc, 8, 128), F32),
            vm((nc, 8, 128), F32),
            vm((nc, 8, 128), F32),
            vm((2, nc, NS * 2 * lt + 1, 8, 128), F32),
            vm((2, nc, NS * 2 * lt + 1, 8, 128), F32),
            vm((2, nc, NS * lt + 1, 8, 128), F32),
            vm((2, nc, NS * lt + 1, 8, 128), F32),
            vm((nc, NS * 2 * lt, 8, 128), F32),
            vm((2, nc, NS * lt // 2 + 1, 8, 128), F32),
            vm((2, nc, NS * lt // 2 + 1, 8, 128), F32),
            vm((2, nc, NS * lt // 4 + 1, 8, 128), F32),
            vm((2, nc, NS * lt // 4 + 1, 8, 128), F32),
            vm((nc, NS * lt // 2, 8, 128), F32),
            dma((NB,)),
            dma((4,)), dma((nc, 4)),
            dma((4,)), dma((nc, 4)),
            dma((4,)), dma((nc, 4)),
            dma((2,)), dma((nc, 2)),
            dma((2,)), dma((nc, 2)),
            dma((2,)), dma((nc, 2)),
            dma((2,)), dma((nc, 2)),
            dma((2,)), dma((nc, 2)),
        ]
        return pl.pallas_call(
            functools.partial(kernel, nc),
            out_shape=jax.ShapeDtypeStruct((nseq, heads, lat), BF16),
            in_specs=[
                pl.BlockSpec(memory_space=pltpu.SMEM),
                pl.BlockSpec(memory_space=pltpu.HBM),
                pl.BlockSpec(memory_space=pltpu.HBM),
            ],
            out_specs=pl.BlockSpec(memory_space=pltpu.VMEM),
            scratch_shapes=scratch,
            compiler_params=pltpu.CompilerParams(collective_id=0, has_side_effects=True, vmem_limit_bytes=56_200_000),
        )(lengths, q, jnp.swapaxes(cache, 1, 2))

    return jax.shard_map(local, mesh=mesh, in_specs=(P('dp', 'dcp', None), P('dp', 'dcp', None), P('dp')),
                         out_specs=P('dp', 'dcp', None), check_vma=False)
```
